512 devices in a mesh: slab: 128 (over z, x, y_hi, core), tm: 4 (over y_lo).
Axes of the slice: x: 4, y: 8 (y_hi: 2, y_lo: 4; y = y_hi * 4 + y_lo), z: 8, core: 2. Of those that a mesh axis runs over, the one named last changes fastest.
Arguments:
- field: float32 [2, 128, 256, 512], P(None, 'slab', None, 'tm'), may hold values from -110 to 110
Outputs:
- evolved: float32 [2, 128, 256, 512], P(None, 'slab', None, 'tm')
The draws below stay inside these ranges and needn't reach their ends.
All inputs are finite; a program needn't handle non-finite values.
Results may differ from the reference program's by a relative error of at most 0.000098.
Values sent between devices are 32-bit elements; how exact they have to be, the bound alone decides.
No kernel may reach another device: no remote copies, remote signals or barrier semaphores. Data moves between devices by JAX's collectives and lax.ppermute only.
A program may use at most 64 MiB of HBM per device.

```python
import math
import jax
import jax.numpy as jnp
from jax import lax

NX = 128
NY = 256
NT = 512


def draw_field(key, part):
    key_rows = jax.random.fold_in(key, 11)
    key_times = jax.random.fold_in(key, 23)
    key_entries = jax.random.fold_in(key, 37)
    log_ten = math.log(10.0)
    rising = 1.0 + 2.0 * jnp.arange(NX, dtype=jnp.float32) / NX
    row_scale = jnp.exp(jax.random.uniform(key_rows, (NX,), jnp.float32, 0.0, log_ten)) * rising
    time_scale = jnp.exp(jax.random.uniform(key_times, (NT,), jnp.float32, 0.0, log_ten))
    entries = jnp.clip(jax.random.normal(key_entries, (2, NX, NY, NT), jnp.float32), -6.0, 6.0)
    amplitude = jnp.sqrt(row_scale[:, None, None] * time_scale[None, None, :])
    return entries * amplitude[None]


def setup_inputs(seed: int = 0) -> dict:
    arg_keys = jax.random.split(jax.random.key(seed), 2)
    field = draw_field(jax.random.fold_in(arg_keys[1], 71), 0)
    return dict(field=field)


TWO_PI = 2.0 * math.pi
DIFFRACT = 4.0
DISPERSE = 3.0
KERR = 0.05
WELL = 1.5
EPSILON = 1e-06

def frequency(length):
    positions = jnp.arange(length, dtype=jnp.int32)
    signed = jnp.where(2 * positions < length, positions, positions - length)
    return signed.astype(jnp.float32) * (TWO_PI / length)

def reference(field):
    mean_power = jnp.mean(field[0] * field[0] + field[1] * field[1])
    launch_scale = 1.0 / jnp.sqrt(mean_power + EPSILON)
    launched = lax.complex(field[0] * launch_scale, field[1] * launch_scale)
    across_x = frequency(NX)
    across_y = frequency(NY)
    temporal = frequency(NT)
    theta = -DIFFRACT * (across_x[:, None, None] ** 2 + across_y[None, :, None] ** 2) + DISPERSE * temporal[None, None, :] ** 2
    rotor = lax.complex(jnp.cos(theta), jnp.sin(theta))

    def half_step(wave):
        return jnp.fft.ifftn(jnp.fft.fftn(wave, axes=(0, 1, 2)) * rotor, axes=(0, 1, 2))
    after_half = half_step(launched)
    place_x = (jnp.arange(NX, dtype=jnp.float32) - (NX - 1) / 2.0) / (NX / 2.0)
    place_y = (jnp.arange(NY, dtype=jnp.float32) - (NY - 1) / 2.0) / (NY / 2.0)
    well_depth = WELL * (place_x[:, None, None] ** 2 + place_y[None, :, None] ** 2)
    intensity = jnp.real(after_half) ** 2 + jnp.imag(after_half) ** 2
    kick_angle = KERR * intensity - well_depth
    kicked = after_half * lax.complex(jnp.cos(kick_angle), jnp.sin(kick_angle))
    evolved = half_step(kicked)
    return jnp.stack([jnp.real(evolved), jnp.imag(evolved)])
```

```python
import math

import jax
import jax.numpy as jnp
import ml_dtypes
import numpy as np
from jax import lax
from jax.experimental import pallas as pl
from jax.experimental.pallas import tpu as pltpu
from jax.sharding import Mesh
from jax.sharding import PartitionSpec as P

NX = 128
NY = 256
NT = 512
SLAB = ("z", "x", "h", "c")
CHIPS = ("z", "x", "h", "t")

TWO_PI = 2.0 * math.pi
DIFFRACT = 4.0
DISPERSE = 3.0
KERR = 0.05
WELL = 1.5
EPSILON = 1e-06


def propagator(length, weight):
    positions = np.arange(length)
    signed = np.where(2 * positions < length, positions, positions - length)
    angle = weight * (signed * (TWO_PI / length)) ** 2
    kernel = np.fft.ifft(np.exp(1j * angle))
    return kernel[(positions[:, None] - positions[None, :]) % length]


def well_phase(length):
    place = (np.arange(length) - (length - 1) / 2.0) / (length / 2.0)
    return np.exp(-1j * WELL * place**2)


def split(matrix):
    full = matrix.astype(np.float32)
    high = full.astype(ml_dtypes.bfloat16)
    low = (matrix - high.astype(np.float64)).astype(ml_dtypes.bfloat16)
    return np.stack([high, low])


def stacked_rows(matrix):
    return split(np.concatenate([matrix.real, matrix.imag], axis=0))


def real_block(matrix):
    return split(np.block([[matrix.real, -matrix.imag], [matrix.imag, matrix.real]]))


def pieces(value):
    high = value.astype(jnp.bfloat16)
    return high, (value - high.astype(jnp.float32)).astype(jnp.bfloat16)


def dot(left, right):
    return jnp.dot(left, right, preferred_element_type=jnp.float32)


def dot_table_left(table_ref, data):
    high, low = pieces(data)
    return dot(table_ref[0], high) + (dot(table_ref[0], low) + dot(table_ref[1], high))


def along_y(real, imag, table_ref):
    r = dot_table_left(table_ref, jnp.concatenate([real, imag], axis=1))
    return r[:NY, :128] - r[NY:, 128:], r[:NY, 128:] + r[NY:, :128]


def along_t(real, imag, table_ref):
    rows = real.shape[0]
    high, low = pieces(jnp.concatenate([real, imag], axis=0))
    both = jnp.concatenate([high, low], axis=0)

    def product(k):
        p = dot(both, table_ref[k, 0])
        return p[: 2 * rows] + (p[2 * rows :] + dot(high, table_ref[k, 1]))

    by_real = product(0)
    by_imag = product(1)
    return by_real[:rows] - by_imag[rows:], by_real[rows:] + by_imag[:rows]


def first_kernel(field_ref, table_ref, out_ref, power_ref):
    real = field_ref[0]
    imag = field_ref[1]
    out_real, out_imag = along_y(real, imag, table_ref)
    out_ref[pl.ds(0, NY, stride=2), :] = out_real
    out_ref[pl.ds(1, NY, stride=2), :] = out_imag
    power = jnp.sum(real * real + imag * imag, axis=0, keepdims=True)
    power_ref[...] = jnp.broadcast_to(power, power_ref.shape)


def time_kernel(core_ref, in_ref, table_ref, keep_ref, send_ref):
    def part(p):
        return jnp.concatenate([in_ref[pl.ds(2 * g + p, NX // 2, stride=8), :] for g in range(4)], axis=1)

    outs = along_t(part(0), part(1), table_ref)
    lower = core_ref[0] == 0
    half = NT // 2
    for p in range(2):
        keep_ref[p] = jnp.where(lower, outs[p][:, :half], outs[p][:, half:])
        send_ref[p] = jnp.where(lower, outs[p][:, half:], outs[p][:, :half])


def kick_kernel(core_ref, keep_in_ref, got_ref, power_ref, table_ref, table2_ref, keep_ref, send_ref):
    lower = core_ref[0] == 0
    rows = []
    for p in range(2):
        rows.append(jnp.where(lower, keep_in_ref[p], got_ref[p]))
        rows.append(jnp.where(lower, got_ref[p], keep_in_ref[p]))
    first = dot_table_left(table_ref, jnp.concatenate(rows, axis=0))
    total = jnp.sum(jnp.sum(power_ref[...], axis=0, keepdims=True), axis=1, keepdims=True)
    scale = 1.0 / jnp.sqrt(total * (1.0 / (NX * NY * NT)) + EPSILON)
    real = first[:NX] * scale
    imag = first[NX:] * scale
    angle = KERR * (real * real + imag * imag)
    cos_turn = jnp.cos(angle)
    sin_turn = jnp.sin(angle)
    kicked = jnp.concatenate([real * cos_turn - imag * sin_turn, real * sin_turn + imag * cos_turn], axis=0)
    second = dot_table_left(table2_ref, kicked)
    half = NX // 2
    for p in range(2):
        even = second[p * NX : p * NX + half]
        odd = second[p * NX + half : (p + 1) * NX]
        keep_ref[p] = jnp.where(lower, even, odd)
        send_ref[p] = jnp.where(lower, odd, even)


def time_back_kernel(core_ref, keep_in_ref, got_ref, table_ref, out_ref):
    lower = core_ref[0] == 0

    def part(p):
        kept = keep_in_ref[p]
        got = got_ref[p]
        return jnp.concatenate([jnp.where(lower, kept, got), jnp.where(lower, got, kept)], axis=1)

    outs = along_t(part(0), part(1), table_ref)
    for p in range(2):
        for g in range(4):
            out_ref[pl.ds(2 * g + p, NX // 2, stride=8), :] = outs[p][:, 128 * g : 128 * (g + 1)]


def last_kernel(in_ref, table_ref, out_ref):
    real = in_ref[pl.ds(0, NY, stride=2), :]
    imag = in_ref[pl.ds(1, NY, stride=2), :]
    out_real, out_imag = along_y(real, imag, table_ref)
    out_ref[0] = out_real
    out_ref[1] = out_imag


def call(kernel, shapes, *args):
    specs = [
        pl.BlockSpec(memory_space=pltpu.SMEM if a.dtype == jnp.int32 else pltpu.VMEM) for a in args
    ]
    outs = [jax.ShapeDtypeStruct(s, jnp.float32) for s in shapes]
    return pl.pallas_call(
        kernel,
        in_specs=specs,
        out_specs=[pl.BlockSpec(memory_space=pltpu.VMEM) for _ in outs],
        out_shape=outs,
        name=kernel.__name__,
    )(*args)


def to_chips(rows):
    moved = lax.all_to_all(rows.reshape(NY, 2, 128), CHIPS, split_axis=0, concat_axis=0, tiled=True)
    return moved.reshape(2 * NY, 128)


def swap(value):
    return lax.ppermute(value, "c", [(0, 1), (1, 0)])


def on_device(field, y_table, y_back, t_table, x_table, x_back):
    core = lax.axis_index("c").astype(jnp.int32).reshape(1)
    rows, power = call(first_kernel, [(2 * NY, 128), (32, 128)], field.reshape(2, NY, 128), y_table)
    moved = to_chips(rows)
    power = lax.all_to_all(power, ("z", "x"), split_axis=0, concat_axis=0, tiled=True)
    power = jnp.broadcast_to(jnp.sum(power, axis=0, keepdims=True), (16, 128))
    power = lax.all_to_all(power, ("h", "c", "t"), split_axis=0, concat_axis=0, tiled=True)
    half = (2, NX // 2, NT // 2)
    keep, send = call(time_kernel, [half, half], core, moved, t_table)
    keep, send = call(kick_kernel, [half, half], core, keep, swap(send), power, x_table, x_back)
    (rows,) = call(time_back_kernel, [(2 * NY, 128)], core, keep, swap(send), t_table)
    (out,) = call(last_kernel, [(2, NY, 128)], to_chips(rows), y_back)
    return out.reshape(2, 1, NY, 128)


def solution(mesh):
    torus = Mesh(mesh.devices.reshape(8, 4, 2, 2, mesh.shape["tm"]), ("z", "x", "h", "c", "t"))
    along_x = propagator(NX, -DIFFRACT)
    order = np.concatenate([np.arange(0, NX, 2), np.arange(1, NX, 2)])
    along_y_matrix = propagator(NY, -DIFFRACT)
    time_matrix = propagator(NT, DISPERSE).T
    tables = (
        stacked_rows(along_y_matrix),
        stacked_rows(along_y_matrix * well_phase(NY)[None, :]),
        np.stack([split(time_matrix.real), split(time_matrix.imag)]),
        real_block(along_x[order][:, order]),
        real_block((along_x * well_phase(NX)[None, :])[order][:, order]),
    )
    placed = P(None, SLAB, None, "t")
    inner = jax.shard_map(
        lambda field: on_device(field, *[jnp.asarray(table) for table in tables]),
        mesh=torus,
        in_specs=(placed,),
        out_specs=placed,
        check_vma=False,
    )
    return inner
```

```python
import math

import jax
import jax.numpy as jnp
import ml_dtypes
import numpy as np
from jax import lax
from jax.experimental import pallas as pl
from jax.experimental.pallas import tpu as pltpu
from jax.sharding import Mesh
from jax.sharding import PartitionSpec as P

NX = 128
NY = 256
NT = 512
HALF_X = NX // 2
SLAB = ("z", "x", "h", "c")
CHIPS = ("z", "x", "h", "t")

TWO_PI = 2.0 * math.pi
DIFFRACT = 4.0
DISPERSE = 3.0
KERR = 0.05
WELL = 1.5
EPSILON = 1e-06


def propagator(length, weight):
    positions = np.arange(length)
    signed = np.where(2 * positions < length, positions, positions - length)
    angle = weight * (signed * (TWO_PI / length)) ** 2
    kernel = np.fft.ifft(np.exp(1j * angle))
    return kernel[(positions[:, None] - positions[None, :]) % length]


def split(matrix):
    full = matrix.astype(np.float32)
    high = full.astype(ml_dtypes.bfloat16)
    low = (matrix - high.astype(np.float64)).astype(ml_dtypes.bfloat16)
    return np.stack([high, low])


def stacked_rows(matrix):
    return split(np.concatenate([matrix.real, matrix.imag], axis=0))


def real_block(matrix):
    return split(np.block([[matrix.real, -matrix.imag], [matrix.imag, matrix.real]]))


def pieces(value):
    high = value.astype(jnp.bfloat16)
    return high, (value - high.astype(jnp.float32)).astype(jnp.bfloat16)


def dot(left, right):
    return jnp.dot(left, right, preferred_element_type=jnp.float32)


def along_y(real, imag, table_ref):
    high, low = pieces(jnp.concatenate([real, imag], axis=1))
    r = dot(table_ref[0], high) + (dot(table_ref[0], low) + dot(table_ref[1], high))
    return r[:NY, :128] - r[NY:, 128:], r[:NY, 128:] + r[NY:, :128]


def along_t(real, imag, table_ref):
    rows = real.shape[0]
    high, low = pieces(jnp.concatenate([real, imag], axis=0))
    both = jnp.concatenate([high, low], axis=0)

    def product(k):
        p = dot(both, table_ref[k, 0])
        return p[: 2 * rows] + (p[2 * rows :] + dot(high, table_ref[k, 1]))

    by_real = product(0)
    by_imag = product(1)
    return by_real[:rows] - by_imag[rows:], by_real[rows:] + by_imag[:rows]


def turns(angle):
    count = jnp.floor(angle * (2.0 / math.pi) + 0.5)
    rest = ((angle - count * 1.5703125) - count * 4.837512969970703125e-4) - count * 7.54978995489188216e-8
    quadrant = count.astype(jnp.int32)
    square = rest * rest
    sine = rest + rest * square * (-1.6666654611e-1 + square * (8.3321608736e-3 - 1.9515295891e-4 * square))
    cosine = (1.0 - 0.5 * square) + square * square * (
        4.166664568298827e-2 + square * (-1.388731625493765e-3 + 2.443315711809948e-5 * square)
    )
    odd = (quadrant & 1) == 1
    cos_turn = jnp.where(odd, sine, cosine)
    sin_turn = jnp.where(odd, cosine, sine)
    return (
        jnp.where(((quadrant + 1) & 2) == 2, -cos_turn, cos_turn),
        jnp.where((quadrant & 2) == 2, -sin_turn, sin_turn),
    )


def first_kernel(field_ref, table_ref, out_ref):
    real = field_ref[0]
    imag = field_ref[1]
    out_real, out_imag = along_y(real, imag, table_ref)
    out_ref[pl.ds(0, NY, stride=3), :] = out_real
    out_ref[pl.ds(1, NY, stride=3), :] = out_imag
    power = jnp.sum(real * real + imag * imag, axis=0, keepdims=True)
    out_ref[pl.ds(2, NY, stride=3), :] = jnp.broadcast_to(power, (NY, 128))


def time_kernel(in_ref, table_ref, out_ref):
    def part(p):
        return jnp.concatenate([in_ref[pl.ds(3 * g + p, HALF_X, stride=12), :] for g in range(4)], axis=1)

    outs = along_t(part(0), part(1), table_ref)
    out_ref[:HALF_X] = outs[0]
    out_ref[HALF_X:NX] = outs[1]
    power = jnp.sum(in_ref[pl.ds(2, NY, stride=3), :], axis=0, keepdims=True)
    out_ref[NX:, :128] = jnp.broadcast_to(power, (8, 128))


def kick_kernel(place_ref, mine_ref, other_ref, x_table_ref, t_table_ref, out_ref, work_ref):
    core = place_ref[0]
    lower = core == 0
    total = jnp.sum(mine_ref[NX : NX + 1, :128] + other_ref[NX : NX + 1, :128], axis=1, keepdims=True)
    scale = 1.0 / jnp.sqrt(total * (1.0 / (NX * NY * NT)) + EPSILON)
    for p in range(2):
        kept = mine_ref[p * HALF_X : (p + 1) * HALF_X]
        got = other_ref[p * HALF_X : (p + 1) * HALF_X]
        work_ref[p * NX : p * NX + HALF_X] = jnp.where(lower, kept, got)
        work_ref[p * NX + HALF_X : (p + 1) * NX] = jnp.where(lower, got, kept)
    high, low = pieces(work_ref[...])
    for parity in range(2):
        table = x_table_ref[0, parity]
        first = dot(table, high) + (dot(table, low) + dot(x_table_ref[1, parity], high))
        for p in range(2):
            work_ref[p * NX + parity * HALF_X : p * NX + (parity + 1) * HALF_X] = first[p * HALF_X : (p + 1) * HALF_X]
    place_y = (place_ref[1].astype(jnp.float32) - (NY - 1) / 2.0) / (NY / 2.0)
    row = lax.broadcasted_iota(jnp.int32, (8, NT), 0)
    for start in range(0, NX, 8):
        parity, base = divmod(start, HALF_X)
        place_x = ((2 * (base + row) + parity).astype(jnp.float32) - (NX - 1) / 2.0) / (NX / 2.0)
        real = work_ref[start : start + 8] * scale
        imag = work_ref[NX + start : NX + start + 8] * scale
        cos_turn, sin_turn = turns(KERR * (real * real + imag * imag) - WELL * (place_x * place_x + place_y * place_y))
        work_ref[start : start + 8] = real * cos_turn - imag * sin_turn
        work_ref[NX + start : NX + start + 8] = real * sin_turn + imag * cos_turn
    high, low = pieces(work_ref[...])
    table = x_table_ref[0, core]
    second = dot(table, high) + (dot(table, low) + dot(x_table_ref[1, core], high))
    outs = along_t(second[:HALF_X], second[HALF_X:], t_table_ref)
    for p in range(2):
        for g in range(4):
            out_ref[pl.ds(2 * g + p, HALF_X, stride=8), :] = outs[p][:, 128 * g : 128 * (g + 1)]


def last_kernel(in_ref, table_ref, out_ref):
    real = in_ref[pl.ds(0, NY, stride=2), :]
    imag = in_ref[pl.ds(1, NY, stride=2), :]
    out_real, out_imag = along_y(real, imag, table_ref)
    out_ref[0] = out_real
    out_ref[1] = out_imag


def call(kernel, shape, *args, scratch=()):
    return pl.pallas_call(
        kernel,
        in_specs=[pl.BlockSpec(memory_space=pltpu.SMEM if a.dtype == jnp.int32 else pltpu.VMEM) for a in args],
        out_specs=pl.BlockSpec(memory_space=pltpu.VMEM),
        out_shape=jax.ShapeDtypeStruct(shape, jnp.float32),
        scratch_shapes=[pltpu.VMEM(s, jnp.float32) for s in scratch],
        compiler_params=pltpu.CompilerParams(vmem_limit_bytes=16 * 2**20),
        name=kernel.__name__,
    )(*args)


def to_chips(rows, count):
    moved = lax.all_to_all(rows.reshape(NY, 1, count * 128), CHIPS, split_axis=0, concat_axis=0, tiled=True)
    return moved.reshape(count * NY, 128)


def on_device(field, y_table, t_table, x_table):
    place = jnp.stack([lax.axis_index("c"), lax.axis_index(CHIPS)]).astype(jnp.int32)
    rows = to_chips(call(first_kernel, (3 * NY, 128), field.reshape(2, NY, 128), y_table), 3)
    mine = call(time_kernel, (NX + 8, NT), rows, t_table)
    other = lax.ppermute(mine, "c", [(0, 1), (1, 0)])
    rows = call(kick_kernel, (2 * NY, 128), place, mine, other, x_table, t_table, scratch=[(2 * NX, NT)])
    out = call(last_kernel, (2, NY, 128), to_chips(rows, 2), y_table)
    return out.reshape(2, 1, NY, 128)


def solution(mesh):
    torus = Mesh(mesh.devices.reshape(8, 4, 2, 2, mesh.shape["tm"]), ("z", "x", "h", "c", "t"))
    along_x = propagator(NX, -DIFFRACT)
    order = np.concatenate([np.arange(0, NX, 2), np.arange(1, NX, 2)])
    along_y_matrix = propagator(NY, -DIFFRACT)
    time_matrix = propagator(NT, DISPERSE).T
    x_block = real_block(along_x[order][:, order])
    x_block = x_block.reshape(2, 2, 2, HALF_X, 2 * NX).transpose(0, 2, 1, 3, 4).reshape(2, 2, NX, 2 * NX)
    tables = (
        stacked_rows(along_y_matrix),
        np.stack([split(time_matrix.real), split(time_matrix.imag)]),
        x_block,
    )
    placed = P(None, SLAB, None, "t")
    inner = jax.shard_map(
        lambda field: on_device(field, *[jnp.asarray(table) for table in tables]),
        mesh=torus,
        in_specs=(placed,),
        out_specs=placed,
        check_vma=False,
    )
    return inner
```

```python
import math

import jax
import jax.numpy as jnp
import ml_dtypes
import numpy as np
from jax import lax
from jax.experimental import pallas as pl
from jax.experimental.pallas import tpu as pltpu
from jax.sharding import Mesh
from jax.sharding import PartitionSpec as P

NX = 128
NY = 256
NT = 512
HALF_X = NX // 2
SLAB = ("z", "x", "h", "c")
CHIPS = ("z", "x", "h", "t")
DEVICES = ("z", "x", "h", "c", "t")
FLIP_X = 37
FLIP = FLIP_X * 4

TWO_PI = 2.0 * math.pi
DIFFRACT = 4.0
DISPERSE = 3.0
KERR = 0.05
WELL = 1.5
EPSILON = 1e-06


def propagator(length, weight):
    positions = np.arange(length)
    signed = np.where(2 * positions < length, positions, positions - length)
    angle = weight * (signed * (TWO_PI / length)) ** 2
    kernel = np.fft.ifft(np.exp(1j * angle))
    return kernel[(positions[:, None] - positions[None, :]) % length]


def split(matrix):
    full = matrix.astype(np.float32)
    high = full.astype(ml_dtypes.bfloat16)
    low = (matrix - high.astype(np.float64)).astype(ml_dtypes.bfloat16)
    return np.stack([high, low])


def stacked_rows(matrix):
    return split(np.concatenate([matrix.real, matrix.imag], axis=0))


def real_block(matrix):
    return split(np.block([[matrix.real, -matrix.imag], [matrix.imag, matrix.real]]))


def pieces(value):
    high = value.astype(jnp.bfloat16)
    return high, (value - high.astype(jnp.float32)).astype(jnp.bfloat16)


def dot(left, right):
    return jnp.dot(left, right, preferred_element_type=jnp.float32)


def along_y(real, imag, table_ref):
    high, low = pieces(jnp.concatenate([real, imag], axis=1))
    r = dot(table_ref[0], high) + (dot(table_ref[0], low) + dot(table_ref[1], high))
    return r[:NY, :128] - r[NY:, 128:], r[:NY, 128:] + r[NY:, :128]


def along_t(real, imag, table_ref):
    rows = real.shape[0]
    high, low = pieces(jnp.concatenate([real, imag], axis=0))
    both = jnp.concatenate([high, low], axis=0)

    def product(k):
        p = dot(both, table_ref[k, 0])
        return p[: 2 * rows] + (p[2 * rows :] + dot(high, table_ref[k, 1]))

    by_real = product(0)
    by_imag = product(1)
    return by_real[:rows] - by_imag[rows:], by_real[rows:] + by_imag[:rows]


def turns(angle):
    count = jnp.floor(angle * (2.0 / math.pi) + 0.5)
    rest = ((angle - count * 1.5703125) - count * 4.837512969970703125e-4) - count * 7.54978995489188216e-8
    quadrant = count.astype(jnp.int32)
    square = rest * rest
    sine = rest + rest * square * (-1.6666654611e-1 + square * (8.3321608736e-3 - 1.9515295891e-4 * square))
    cosine = (1.0 - 0.5 * square) + square * square * (
        4.166664568298827e-2 + square * (-1.388731625493765e-3 + 2.443315711809948e-5 * square)
    )
    odd = (quadrant & 1) == 1
    cos_turn = jnp.where(odd, sine, cosine)
    sin_turn = jnp.where(odd, cosine, sine)
    return (
        jnp.where(((quadrant + 1) & 2) == 2, -cos_turn, cos_turn),
        jnp.where((quadrant & 2) == 2, -sin_turn, sin_turn),
    )


def first_kernel(field_ref, table_ref, out_ref):
    real = field_ref[0]
    imag = field_ref[1]
    out_real, out_imag = along_y(real, imag, table_ref)
    out_ref[pl.ds(0, NY, stride=3), :] = out_real
    out_ref[pl.ds(1, NY, stride=3), :] = out_imag
    power = jnp.sum(real * real + imag * imag, axis=0, keepdims=True)
    out_ref[pl.ds(2, NY, stride=3), :] = jnp.broadcast_to(power, (NY, 128))


def time_kernel(in_ref, table_ref, out_ref):
    def part(p):
        return jnp.concatenate([in_ref[pl.ds(3 * g + p, HALF_X, stride=12), :] for g in range(4)], axis=1)

    outs = along_t(part(0), part(1), table_ref)
    out_ref[:HALF_X] = outs[0]
    out_ref[HALF_X:NX] = outs[1]
    power = jnp.sum(in_ref[pl.ds(2, NY, stride=3), :], axis=0, keepdims=True)
    out_ref[NX:, :128] = jnp.broadcast_to(power, (8, 128))


def kick_kernel(place_ref, mine_ref, other_ref, x_table_ref, t_table_ref, out_ref, work_ref):
    core = place_ref[0]
    lower = core == 0
    total = jnp.sum(mine_ref[NX : NX + 1, :128] + other_ref[NX : NX + 1, :128], axis=1, keepdims=True)
    scale = 1.0 / jnp.sqrt(total * (1.0 / (NX * NY * NT)) + EPSILON)
    for p in range(2):
        kept = mine_ref[p * HALF_X : (p + 1) * HALF_X]
        got = other_ref[p * HALF_X : (p + 1) * HALF_X]
        work_ref[p * NX : p * NX + HALF_X] = jnp.where(lower, kept, got)
        work_ref[p * NX + HALF_X : (p + 1) * NX] = jnp.where(lower, got, kept)
    high, low = pieces(work_ref[...])
    for parity in range(2):
        table = x_table_ref[0, parity]
        first = dot(table, high) + (dot(table, low) + dot(x_table_ref[1, parity], high))
        for p in range(2):
            work_ref[p * NX + parity * HALF_X : p * NX + (parity + 1) * HALF_X] = first[p * HALF_X : (p + 1) * HALF_X]
    place_y = (place_ref[1].astype(jnp.float32) - (NY - 1) / 2.0) / (NY / 2.0)
    row = lax.broadcasted_iota(jnp.int32, (8, NT), 0)
    for start in range(0, NX, 8):
        parity, base = divmod(start, HALF_X)
        place_x = ((2 * ((base + row) ^ FLIP_X) + parity).astype(jnp.float32) - (NX - 1) / 2.0) / (NX / 2.0)
        real = work_ref[start : start + 8] * scale
        imag = work_ref[NX + start : NX + start + 8] * scale
        cos_turn, sin_turn = turns(KERR * (real * real + imag * imag) - WELL * (place_x * place_x + place_y * place_y))
        work_ref[start : start + 8] = real * cos_turn - imag * sin_turn
        work_ref[NX + start : NX + start + 8] = real * sin_turn + imag * cos_turn
    high, low = pieces(work_ref[...])
    table = x_table_ref[0, core]
    second = dot(table, high) + (dot(table, low) + dot(x_table_ref[1, core], high))
    outs = along_t(second[:HALF_X], second[HALF_X:], t_table_ref)
    for p in range(2):
        for g in range(4):
            out_ref[pl.ds(2 * g + p, HALF_X, stride=8), :] = outs[p][:, 128 * g : 128 * (g + 1)]


def last_kernel(in_ref, table_ref, out_ref):
    real = in_ref[pl.ds(0, NY, stride=2), :]
    imag = in_ref[pl.ds(1, NY, stride=2), :]
    out_real, out_imag = along_y(real, imag, table_ref)
    out_ref[0] = out_real
    out_ref[1] = out_imag


def call(kernel, shape, *args, scratch=()):
    return pl.pallas_call(
        kernel,
        in_specs=[pl.BlockSpec(memory_space=pltpu.SMEM if a.dtype == jnp.int32 else pltpu.VMEM) for a in args],
        out_specs=pl.BlockSpec(memory_space=pltpu.VMEM),
        out_shape=jax.ShapeDtypeStruct(shape, jnp.float32),
        scratch_shapes=[pltpu.VMEM(s, jnp.float32) for s in scratch],
        compiler_params=pltpu.CompilerParams(vmem_limit_bytes=16 * 2**20),
        name=kernel.__name__,
    )(*args)


def groups():
    found = []
    for core in range(2):
        chips = [position ^ FLIP for position in range(NY)]
        found.append([(chip >> 2) * 8 + core * 4 + (chip & 3) for chip in chips])
    return found


def to_chips(rows, count):
    moved = lax.all_to_all(
        rows.reshape(NY, 1, count * 128),
        DEVICES,
        split_axis=0,
        concat_axis=0,
        tiled=True,
        axis_index_groups=groups(),
    )
    return moved.reshape(count * NY, 128)


def on_device(field, y_table, t_table, x_table):
    place = jnp.stack([lax.axis_index("c"), lax.axis_index(CHIPS) ^ FLIP]).astype(jnp.int32)
    rows = to_chips(call(first_kernel, (3 * NY, 128), field.reshape(2, NY, 128), y_table), 3)
    mine = call(time_kernel, (NX + 8, NT), rows, t_table)
    other = lax.ppermute(mine, "c", [(0, 1), (1, 0)])
    rows = call(kick_kernel, (2 * NY, 128), place, mine, other, x_table, t_table, scratch=[(2 * NX, NT)])
    out = call(last_kernel, (2, NY, 128), to_chips(rows, 2), y_table)
    return out.reshape(2, 1, NY, 128)


def solution(mesh):
    torus = Mesh(mesh.devices.reshape(8, 4, 2, 2, mesh.shape["tm"]), ("z", "x", "h", "c", "t"))
    along_x = propagator(NX, -DIFFRACT)
    even = 2 * (np.arange(HALF_X) ^ FLIP_X)
    order = np.concatenate([even, even + 1])
    along_y_matrix = propagator(NY, -DIFFRACT)
    time_matrix = propagator(NT, DISPERSE).T
    x_block = real_block(along_x[order][:, order])
    x_block = x_block.reshape(2, 2, 2, HALF_X, 2 * NX).transpose(0, 2, 1, 3, 4).reshape(2, 2, NX, 2 * NX)
    tables = (
        stacked_rows(along_y_matrix),
        np.stack([split(time_matrix.real), split(time_matrix.imag)]),
        x_block,
    )
    placed = P(None, SLAB, None, "t")
    inner = jax.shard_map(
        lambda field: on_device(field, *[jnp.asarray(table) for table in tables]),
        mesh=torus,
        in_specs=(placed,),
        out_specs=placed,
        check_vma=False,
    )
    return inner
```

```python
import math

import jax
import jax.numpy as jnp
import ml_dtypes
import numpy as np
from jax import lax
from jax.experimental import pallas as pl
from jax.experimental.pallas import tpu as pltpu
from jax.sharding import Mesh
from jax.sharding import PartitionSpec as P

NX = 128
NY = 256
NT = 512
HALF_X = NX // 2
SLAB = ("z", "x", "h", "c")
CHIPS = ("z", "x", "h", "t")
DEVICES = ("z", "x", "h", "c", "t")
EXTENT = (8, 4, 8)
ROOT = (4, 2, 4)
HOP = (0.46, 0.41, 0.54)

TWO_PI = 2.0 * math.pi
DIFFRACT = 4.0
DISPERSE = 3.0
KERR = 0.05
WELL = 1.5
EPSILON = 1e-06


def propagator(length, weight):
    positions = np.arange(length)
    signed = np.where(2 * positions < length, positions, positions - length)
    angle = weight * (signed * (TWO_PI / length)) ** 2
    kernel = np.fft.ifft(np.exp(1j * angle))
    return kernel[(positions[:, None] - positions[None, :]) % length]


def split(matrix):
    full = matrix.astype(np.float32)
    high = full.astype(ml_dtypes.bfloat16)
    low = (matrix - high.astype(np.float64)).astype(ml_dtypes.bfloat16)
    return np.stack([high, low])


def run_order():
    def cost(run):
        place = (run >> 3, (run >> 1) & 3, 4 * (run & 1))
        away = [abs(p - r) for p, r in zip(place, ROOT)]
        return sum(w * min(d, n - d) for w, d, n in zip(HOP, away, EXTENT))

    root = ROOT[0] * 8 + ROOT[1] * 2 + ROOT[2] // 4
    return [root] + sorted((run for run in range(HALF_X) if run != root), key=lambda run: (-cost(run), run))


def real_block(matrix):
    return split(np.block([[matrix.real, -matrix.imag], [matrix.imag, matrix.real]]))


def pieces(value):
    high = value.astype(jnp.bfloat16)
    return high, (value - high.astype(jnp.float32)).astype(jnp.bfloat16)


def dot(left, right):
    return jnp.dot(left, right, preferred_element_type=jnp.float32)


def along_y(real, imag, table_ref):
    straight = jnp.concatenate([real, imag], axis=1)
    half = NY // 2
    data = jnp.concatenate([straight, jnp.concatenate([straight[half:], straight[:half]], axis=0)], axis=1)
    high, low = pieces(data)
    r = dot(table_ref[0], high) + (dot(table_ref[0], low) + dot(table_ref[1], high))
    by_real = r[:half]
    by_imag = r[half:]
    reals = [by_real[:, j : j + 128] - by_imag[:, j + 128 : j + 256] for j in (0, 256)]
    imags = [by_real[:, j + 128 : j + 256] + by_imag[:, j : j + 128] for j in (0, 256)]
    return reals, imags


def along_t(blocks, table_ref):
    rows = blocks[0][0].shape[0]
    split_blocks = [[pieces(block) for block in part] for part in blocks]

    def pairs(k):
        return jnp.concatenate(
            [
                jnp.concatenate([split_blocks[p][g][k], split_blocks[p][(g + 1) % 4][k]], axis=1)
                for g in range(4)
                for p in range(2)
            ],
            axis=0,
        )

    high, low = pairs(0), pairs(1)
    r = dot(high, table_ref[0]) + (dot(low, table_ref[0]) + dot(high, table_ref[1]))

    def product(g, p):
        upper = (2 * g + p) * rows
        lower = (2 * ((g + 2) % 4) + p) * rows
        return r[upper : upper + rows, :256] + r[lower : lower + rows, 256:]

    outs = [[], []]
    for g in range(4):
        from_real = product(g, 0)
        from_imag = product(g, 1)
        outs[0].append(from_real[:, :128] - from_imag[:, 128:])
        outs[1].append(from_imag[:, :128] + from_real[:, 128:])
    return outs


def turns(angle):
    count = jnp.floor(angle * (2.0 / math.pi) + 0.5)
    rest = ((angle - count * 1.5703125) - count * 4.837512969970703125e-4) - count * 7.54978995489188216e-8
    quadrant = count.astype(jnp.int32)
    square = rest * rest
    sine = rest + rest * square * (-1.6666654611e-1 + square * (8.3321608736e-3 - 1.9515295891e-4 * square))
    cosine = (1.0 - 0.5 * square) + square * square * (
        4.166664568298827e-2 + square * (-1.388731625493765e-3 + 2.443315711809948e-5 * square)
    )
    odd = (quadrant & 1) == 1
    cos_turn = jnp.where(odd, sine, cosine)
    sin_turn = jnp.where(odd, cosine, sine)
    return (
        jnp.where(((quadrant + 1) & 2) == 2, -cos_turn, cos_turn),
        jnp.where((quadrant & 2) == 2, -sin_turn, sin_turn),
    )


def first_kernel(field_hbm, table_hbm, out_ref, field_ref, table_ref, sems):
    copies = [
        pltpu.make_async_copy(field_hbm, field_ref, sems.at[0]),
        pltpu.make_async_copy(table_hbm, table_ref, sems.at[1]),
    ]
    for copy in copies:
        copy.start()
    for copy in copies:
        copy.wait()
    real = field_ref[0]
    imag = field_ref[1]
    reals, imags = along_y(real, imag, table_ref)
    half = NY // 2
    for j in range(2):
        out_ref[pl.ds(3 * half * j, half, stride=3), :] = reals[j]
        out_ref[pl.ds(3 * half * j + 1, half, stride=3), :] = imags[j]
    power = jnp.sum(real * real + imag * imag, axis=0, keepdims=True)
    out_ref[pl.ds(2, NY, stride=3), :] = jnp.broadcast_to(power, (NY, 128))


def time_kernel(in_ref, table_ref, out_ref):
    blocks = [[in_ref[pl.ds(3 * g + p, HALF_X, stride=12), :] for g in range(4)] for p in range(2)]
    outs = along_t(blocks, table_ref)
    for p in range(2):
        for g in range(4):
            out_ref[p * HALF_X : (p + 1) * HALF_X, 128 * g : 128 * (g + 1)] = outs[p][g]
    power = jnp.sum(in_ref[pl.ds(2, NY, stride=3), :], axis=0, keepdims=True)
    out_ref[NX:, :128] = jnp.broadcast_to(power, (8, 128))


def kick_kernel(place_ref, position_ref, mine_ref, other_ref, well_ref, x_table_ref, t_table_ref, out_ref, work_ref):
    core = place_ref[0]
    lower = core == 0
    total = jnp.sum(mine_ref[NX : NX + 1, :128] + other_ref[NX : NX + 1, :128], axis=1, keepdims=True)
    scale = 1.0 / jnp.sqrt(total * (1.0 / (NX * NY * NT)) + EPSILON)
    for p in range(2):
        kept = mine_ref[p * HALF_X : (p + 1) * HALF_X]
        got = other_ref[p * HALF_X : (p + 1) * HALF_X]
        work_ref[p * NX : p * NX + HALF_X] = jnp.where(lower, kept, got)
        work_ref[p * NX + HALF_X : (p + 1) * NX] = jnp.where(lower, got, kept)
    high, low = pieces(work_ref[...])
    for parity in range(2):
        table = x_table_ref[0, parity]
        first = dot(table, high) + (dot(table, low) + dot(x_table_ref[1, parity], high))
        for p in range(2):
            work_ref[p * NX + parity * HALF_X : p * NX + (parity + 1) * HALF_X] = first[p * HALF_X : (p + 1) * HALF_X]
    place_y = (position_ref[place_ref[1]].astype(jnp.float32) - (NY - 1) / 2.0) / (NY / 2.0)
    well_y = WELL * place_y * place_y
    for start in range(0, NX, 8):
        well = jnp.concatenate([well_ref[start : start + 8] + well_y] * 4, axis=1)
        real = work_ref[start : start + 8] * scale
        imag = work_ref[NX + start : NX + start + 8] * scale
        cos_turn, sin_turn = turns(KERR * (real * real + imag * imag) - well)
        work_ref[start : start + 8] = real * cos_turn - imag * sin_turn
        work_ref[NX + start : NX + start + 8] = real * sin_turn + imag * cos_turn
    high, low = pieces(work_ref[...])
    table = x_table_ref[0, core]
    second = dot(table, high) + (dot(table, low) + dot(x_table_ref[1, core], high))
    blocks = [[second[p * HALF_X : (p + 1) * HALF_X, 128 * g : 128 * (g + 1)] for g in range(4)] for p in range(2)]
    outs = along_t(blocks, t_table_ref)
    for p in range(2):
        for g in range(4):
            out_ref[pl.ds(2 * g + p, HALF_X, stride=8), :] = outs[p][g]


def last_kernel(in_ref, table_ref, out_ref):
    real = in_ref[pl.ds(0, NY, stride=2), :]
    imag = in_ref[pl.ds(1, NY, stride=2), :]
    reals, imags = along_y(real, imag, table_ref)
    half = NY // 2
    for j in range(2):
        out_ref[0, j * half : (j + 1) * half] = reals[j]
        out_ref[1, j * half : (j + 1) * half] = imags[j]


def call(kernel, shape, *args, scratch=(), direct=False):
    def place(a):
        if a.dtype == jnp.int32:
            return pltpu.SMEM
        return pltpu.HBM if direct else pltpu.VMEM

    return pl.pallas_call(
        kernel,
        in_specs=[pl.BlockSpec(memory_space=place(a)) for a in args],
        out_specs=pl.BlockSpec(memory_space=pltpu.VMEM),
        out_shape=jax.ShapeDtypeStruct(shape, jnp.float32),
        scratch_shapes=list(scratch),
        compiler_params=pltpu.CompilerParams(vmem_limit_bytes=16 * 2**20),
        name=kernel.__name__,
    )(*args)


def groups():
    return [[run * 8 + core * 4 + t for run in run_order() for t in range(4)] for core in range(2)]


def to_chips(rows, count):
    moved = lax.all_to_all(
        rows.reshape(NY, 1, count * 128),
        DEVICES,
        split_axis=0,
        concat_axis=0,
        tiled=True,
        axis_index_groups=groups(),
    )
    return moved.reshape(count * NY, 128)


def on_device(field, y_table, t_table, x_table, well, positions):
    place = jnp.stack([lax.axis_index("c"), lax.axis_index(CHIPS)]).astype(jnp.int32)
    scratch = [pltpu.VMEM((2, NY, 128), jnp.float32), pltpu.VMEM(y_table.shape, jnp.bfloat16), pltpu.SemaphoreType.DMA((2,))]
    from_hbm = [pltpu.with_memory_space_constraint(a, pltpu.HBM) for a in (field.reshape(2, NY, 128), y_table)]
    rows = call(first_kernel, (3 * NY, 128), *from_hbm, scratch=scratch, direct=True)
    mine = call(time_kernel, (NX + 8, NT), to_chips(rows, 3), t_table)
    other = lax.ppermute(mine, "c", [(0, 1), (1, 0)])
    scratch = [pltpu.VMEM((2 * NX, NT), jnp.float32)]
    rows = call(kick_kernel, (2 * NY, 128), place, positions, mine, other, well, x_table, t_table, scratch=scratch)
    out = call(last_kernel, (2, NY, 128), to_chips(rows, 2), y_table)
    return out.reshape(2, 1, NY, 128)


def solution(mesh):
    torus = Mesh(mesh.devices.reshape(8, 4, 2, 2, mesh.shape["tm"]), DEVICES)
    runs = np.array(run_order())
    order = np.concatenate([2 * runs, 2 * runs + 1])
    positions = np.empty((NY,), np.int32)
    positions[(4 * runs[:, None] + np.arange(4)).reshape(-1)] = np.arange(NY)
    along_x = propagator(NX, -DIFFRACT)
    y_rows = propagator(NY, -DIFFRACT)[: NY // 2]
    t_columns = propagator(NT, DISPERSE).T[:, :128]
    t_columns = np.concatenate([t_columns.real, t_columns.imag], axis=1)
    x_block = real_block(along_x[order][:, order])
    place_x = (order - (NX - 1) / 2.0) / (NX / 2.0)
    tables = (
        split(np.concatenate([y_rows.real, y_rows.imag], axis=0)),
        split(np.concatenate([t_columns[: NT // 2], t_columns[NT // 2 :]], axis=1)),
        x_block.reshape(2, 2, 2, HALF_X, 2 * NX).transpose(0, 2, 1, 3, 4).reshape(2, 2, NX, 2 * NX),
        np.broadcast_to((WELL * place_x**2).astype(np.float32)[:, None], (NX, 128)),
        positions,
    )
    placed = P(None, SLAB, None, "t")
    inner = jax.shard_map(
        lambda field: on_device(field, *[jnp.asarray(table) for table in tables]),
        mesh=torus,
        in_specs=(placed,),
        out_specs=placed,
        check_vma=False,
    )
    return inner
```

```python
import math

import jax
import jax.numpy as jnp
import ml_dtypes
import numpy as np
from jax import lax
from jax.experimental import pallas as pl
from jax.experimental.pallas import tpu as pltpu
from jax.sharding import Mesh
from jax.sharding import PartitionSpec as P

NX = 128
NY = 256
NT = 512
HALF_X = NX // 2
SLAB = ("z", "x", "h", "c")
CHIPS = ("z", "x", "h", "t")
DEVICES = ("z", "x", "h", "c", "t")
EXTENT = (8, 4, 8)
ROOT = (4, 2, 4)
STEP = 1.02
HOP = (0.47, 0.45, 0.62)

TWO_PI = 2.0 * math.pi
DIFFRACT = 4.0
DISPERSE = 3.0
KERR = 0.05
WELL = 1.5
EPSILON = 1e-06


def propagator(length, weight):
    positions = np.arange(length)
    signed = np.where(2 * positions < length, positions, positions - length)
    angle = weight * (signed * (TWO_PI / length)) ** 2
    kernel = np.fft.ifft(np.exp(1j * angle))
    return kernel[(positions[:, None] - positions[None, :]) % length]


def split(matrix):
    full = matrix.astype(np.float32)
    high = full.astype(ml_dtypes.bfloat16)
    low = (matrix - high.astype(np.float64)).astype(ml_dtypes.bfloat16)
    return np.stack([high, low])


def run_order():
    def start(run):
        place = (run >> 3, (run >> 1) & 3, 4 * (run & 1) + 1.5)
        return STEP * place[0] + sum(w * min(p, n - p) for w, p, n in zip(HOP, place, EXTENT))

    root = ROOT[0] * 8 + ROOT[1] * 2 + ROOT[2] // 4
    return [root] + sorted((run for run in range(HALF_X) if run != root), key=lambda run: (-start(run), run))


def real_block(matrix):
    return split(np.block([[matrix.real, -matrix.imag], [matrix.imag, matrix.real]]))


def pieces(value):
    high = value.astype(jnp.bfloat16)
    return high, (value - high.astype(jnp.float32)).astype(jnp.bfloat16)


def dot(left, right):
    return jnp.dot(left, right, preferred_element_type=jnp.float32)


def along_y(real, imag, table_ref):
    straight = jnp.concatenate([real, imag], axis=1)
    half = NY // 2
    data = jnp.concatenate([straight, jnp.concatenate([straight[half:], straight[:half]], axis=0)], axis=1)
    high, low = pieces(data)
    r = dot(table_ref[0], high) + (dot(table_ref[0], low) + dot(table_ref[1], high))
    by_real = r[:half]
    by_imag = r[half:]
    reals = [by_real[:, j : j + 128] - by_imag[:, j + 128 : j + 256] for j in (0, 256)]
    imags = [by_real[:, j + 128 : j + 256] + by_imag[:, j : j + 128] for j in (0, 256)]
    return reals, imags


def along_t(blocks, table_ref):
    rows = blocks[0][0].shape[0]
    split_blocks = [[pieces(block) for block in part] for part in blocks]

    def pairs(k):
        return jnp.concatenate(
            [
                jnp.concatenate([split_blocks[p][g][k], split_blocks[p][(g + 1) % 4][k]], axis=1)
                for g in range(4)
                for p in range(2)
            ],
            axis=0,
        )

    high, low = pairs(0), pairs(1)
    r = dot(high, table_ref[0]) + (dot(low, table_ref[0]) + dot(high, table_ref[1]))

    def product(g, p):
        upper = (2 * g + p) * rows
        lower = (2 * ((g + 2) % 4) + p) * rows
        return r[upper : upper + rows, :256] + r[lower : lower + rows, 256:]

    outs = [[], []]
    for g in range(4):
        from_real = product(g, 0)
        from_imag = product(g, 1)
        outs[0].append(from_real[:, :128] - from_imag[:, 128:])
        outs[1].append(from_imag[:, :128] + from_real[:, 128:])
    return outs


def turns(angle):
    count = jnp.floor(angle * (2.0 / math.pi) + 0.5)
    rest = ((angle - count * 1.5703125) - count * 4.837512969970703125e-4) - count * 7.54978995489188216e-8
    quadrant = count.astype(jnp.int32)
    square = rest * rest
    sine = rest + rest * square * (-1.6666654611e-1 + square * (8.3321608736e-3 - 1.9515295891e-4 * square))
    cosine = (1.0 - 0.5 * square) + square * square * (
        4.166664568298827e-2 + square * (-1.388731625493765e-3 + 2.443315711809948e-5 * square)
    )
    odd = (quadrant & 1) == 1
    cos_turn = jnp.where(odd, sine, cosine)
    sin_turn = jnp.where(odd, cosine, sine)
    return (
        jnp.where(((quadrant + 1) & 2) == 2, -cos_turn, cos_turn),
        jnp.where((quadrant & 2) == 2, -sin_turn, sin_turn),
    )


def first_kernel(field_hbm, table_hbm, out_ref, field_ref, table_ref, sems):
    copies = [
        pltpu.make_async_copy(field_hbm, field_ref, sems.at[0]),
        pltpu.make_async_copy(table_hbm, table_ref, sems.at[1]),
    ]
    for copy in copies:
        copy.start()
    for copy in copies:
        copy.wait()
    real = field_ref[0]
    imag = field_ref[1]
    reals, imags = along_y(real, imag, table_ref)
    half = NY // 2
    for j in range(2):
        out_ref[pl.ds(3 * half * j, half, stride=3), :] = reals[j]
        out_ref[pl.ds(3 * half * j + 1, half, stride=3), :] = imags[j]
    power = jnp.sum(real * real + imag * imag, axis=0, keepdims=True)
    out_ref[pl.ds(2, NY, stride=3), :] = jnp.broadcast_to(power, (NY, 128))


def time_kernel(in_ref, table_ref, out_ref):
    blocks = [[in_ref[pl.ds(3 * g + p, HALF_X, stride=12), :] for g in range(4)] for p in range(2)]
    outs = along_t(blocks, table_ref)
    for p in range(2):
        for g in range(4):
            out_ref[p * HALF_X : (p + 1) * HALF_X, 128 * g : 128 * (g + 1)] = outs[p][g]
    power = jnp.sum(in_ref[pl.ds(2, NY, stride=3), :], axis=0, keepdims=True)
    out_ref[NX:, :128] = jnp.broadcast_to(power, (8, 128))


def kick_kernel(place_ref, position_ref, mine_ref, other_ref, well_ref, x_table_ref, t_table_ref, out_ref, work_ref):
    core = place_ref[0]
    lower = core == 0
    total = jnp.sum(mine_ref[NX : NX + 1, :128] + other_ref[NX : NX + 1, :128], axis=1, keepdims=True)
    scale = 1.0 / jnp.sqrt(total * (1.0 / (NX * NY * NT)) + EPSILON)
    for p in range(2):
        kept = mine_ref[p * HALF_X : (p + 1) * HALF_X]
        got = other_ref[p * HALF_X : (p + 1) * HALF_X]
        work_ref[p * NX : p * NX + HALF_X] = jnp.where(lower, kept, got)
        work_ref[p * NX + HALF_X : (p + 1) * NX] = jnp.where(lower, got, kept)
    high, low = pieces(work_ref[...])
    for parity in range(2):
        table = x_table_ref[0, parity]
        first = dot(table, high) + (dot(table, low) + dot(x_table_ref[1, parity], high))
        for p in range(2):
            work_ref[p * NX + parity * HALF_X : p * NX + (parity + 1) * HALF_X] = first[p * HALF_X : (p + 1) * HALF_X]
    place_y = (position_ref[place_ref[1]].astype(jnp.float32) - (NY - 1) / 2.0) / (NY / 2.0)
    well_y = WELL * place_y * place_y
    for start in range(0, NX, 8):
        well = jnp.concatenate([well_ref[start : start + 8] + well_y] * 4, axis=1)
        real = work_ref[start : start + 8] * scale
        imag = work_ref[NX + start : NX + start + 8] * scale
        cos_turn, sin_turn = turns(KERR * (real * real + imag * imag) - well)
        work_ref[start : start + 8] = real * cos_turn - imag * sin_turn
        work_ref[NX + start : NX + start + 8] = real * sin_turn + imag * cos_turn
    high, low = pieces(work_ref[...])
    table = x_table_ref[0, core]
    second = dot(table, high) + (dot(table, low) + dot(x_table_ref[1, core], high))
    blocks = [[second[p * HALF_X : (p + 1) * HALF_X, 128 * g : 128 * (g + 1)] for g in range(4)] for p in range(2)]
    outs = along_t(blocks, t_table_ref)
    for p in range(2):
        for g in range(4):
            out_ref[pl.ds(2 * g + p, HALF_X, stride=8), :] = outs[p][g]


def last_kernel(in_ref, table_ref, out_ref):
    real = in_ref[pl.ds(0, NY, stride=2), :]
    imag = in_ref[pl.ds(1, NY, stride=2), :]
    reals, imags = along_y(real, imag, table_ref)
    half = NY // 2
    for j in range(2):
        out_ref[0, j * half : (j + 1) * half] = reals[j]
        out_ref[1, j * half : (j + 1) * half] = imags[j]


def call(kernel, shape, *args, scratch=(), direct=False):
    def place(a):
        if a.dtype == jnp.int32:
            return pltpu.SMEM
        return pltpu.HBM if direct else pltpu.VMEM

    return pl.pallas_call(
        kernel,
        in_specs=[pl.BlockSpec(memory_space=place(a)) for a in args],
        out_specs=pl.BlockSpec(memory_space=pltpu.VMEM),
        out_shape=jax.ShapeDtypeStruct(shape, jnp.float32),
        scratch_shapes=list(scratch),
        compiler_params=pltpu.CompilerParams(vmem_limit_bytes=16 * 2**20),
        name=kernel.__name__,
    )(*args)


def groups():
    return [[run * 8 + core * 4 + t for run in run_order() for t in range(4)] for core in range(2)]


def to_chips(rows, count):
    moved = lax.all_to_all(
        rows.reshape(NY, 1, count * 128),
        DEVICES,
        split_axis=0,
        concat_axis=0,
        tiled=True,
        axis_index_groups=groups(),
    )
    return moved.reshape(count * NY, 128)


def on_device(field, y_table, t_table, x_table, well, positions):
    place = jnp.stack([lax.axis_index("c"), lax.axis_index(CHIPS)]).astype(jnp.int32)
    scratch = [pltpu.VMEM((2, NY, 128), jnp.float32), pltpu.VMEM(y_table.shape, jnp.bfloat16), pltpu.SemaphoreType.DMA((2,))]
    from_hbm = [pltpu.with_memory_space_constraint(a, pltpu.HBM) for a in (field.reshape(2, NY, 128), y_table)]
    rows = call(first_kernel, (3 * NY, 128), *from_hbm, scratch=scratch, direct=True)
    mine = call(time_kernel, (NX + 8, NT), to_chips(rows, 3), t_table)
    other = lax.ppermute(mine, "c", [(0, 1), (1, 0)])
    scratch = [pltpu.VMEM((2 * NX, NT), jnp.float32)]
    rows = call(kick_kernel, (2 * NY, 128), place, positions, mine, other, well, x_table, t_table, scratch=scratch)
    out = call(last_kernel, (2, NY, 128), to_chips(rows, 2), y_table)
    return out.reshape(2, 1, NY, 128)


def solution(mesh):
    torus = Mesh(mesh.devices.reshape(8, 4, 2, 2, mesh.shape["tm"]), DEVICES)
    runs = np.array(run_order())
    order = np.concatenate([2 * runs, 2 * runs + 1])
    positions = np.empty((NY,), np.int32)
    positions[(4 * runs[:, None] + np.arange(4)).reshape(-1)] = np.arange(NY)
    along_x = propagator(NX, -DIFFRACT)
    y_rows = propagator(NY, -DIFFRACT)[: NY // 2]
    t_columns = propagator(NT, DISPERSE).T[:, :128]
    t_columns = np.concatenate([t_columns.real, t_columns.imag], axis=1)
    x_block = real_block(along_x[order][:, order])
    place_x = (order - (NX - 1) / 2.0) / (NX / 2.0)
    tables = (
        split(np.concatenate([y_rows.real, y_rows.imag], axis=0)),
        split(np.concatenate([t_columns[: NT // 2], t_columns[NT // 2 :]], axis=1)),
        x_block.reshape(2, 2, 2, HALF_X, 2 * NX).transpose(0, 2, 1, 3, 4).reshape(2, 2, NX, 2 * NX),
        np.broadcast_to((WELL * place_x**2).astype(np.float32)[:, None], (NX, 128)),
        positions,
    )
    placed = P(None, SLAB, None, "t")
    inner = jax.shard_map(
        lambda field: on_device(field, *[jnp.asarray(table) for table in tables]),
        mesh=torus,
        in_specs=(placed,),
        out_specs=placed,
        check_vma=False,
    )
    return inner
```

```python
import math

import jax
import jax.numpy as jnp
import ml_dtypes
import numpy as np
from jax import lax
from jax.experimental import pallas as pl
from jax.experimental.pallas import tpu as pltpu
from jax.sharding import Mesh
from jax.sharding import PartitionSpec as P

NX = 128
NY = 256
NT = 512
HALF_X = NX // 2
SLAB = ("z", "x", "h", "c")
CHIPS = ("z", "x", "h", "t")
DEVICES = ("z", "x", "h", "c", "t")
FLIP_X = 37
FLIP = 4 * FLIP_X

TWO_PI = 2.0 * math.pi
DIFFRACT = 4.0
DISPERSE = 3.0
KERR = 0.05
WELL = 1.5
EPSILON = 1e-06


def propagator(length, weight):
    positions = np.arange(length)
    signed = np.where(2 * positions < length, positions, positions - length)
    angle = weight * (signed * (TWO_PI / length)) ** 2
    kernel = np.fft.ifft(np.exp(1j * angle))
    return kernel[(positions[:, None] - positions[None, :]) % length]


def split(matrix):
    full = matrix.astype(np.float32)
    high = full.astype(ml_dtypes.bfloat16)
    low = (matrix - high.astype(np.float64)).astype(ml_dtypes.bfloat16)
    return np.stack([high, low])


def real_block(matrix):
    return split(np.block([[matrix.real, -matrix.imag], [matrix.imag, matrix.real]]))


def pieces(value):
    high = value.astype(jnp.bfloat16)
    return high, (value - high.astype(jnp.float32)).astype(jnp.bfloat16)


def dot(left, right):
    return jnp.dot(left, right, preferred_element_type=jnp.float32)


def along_y(real, imag, table_ref):
    straight = jnp.concatenate([real, imag], axis=1)
    half = NY // 2
    data = jnp.concatenate([straight, jnp.concatenate([straight[half:], straight[:half]], axis=0)], axis=1)
    high, low = pieces(data)
    r = dot(table_ref[0], high) + (dot(table_ref[0], low) + dot(table_ref[1], high))
    by_real = r[:half]
    by_imag = r[half:]
    reals = [by_real[:, j : j + 128] - by_imag[:, j + 128 : j + 256] for j in (0, 256)]
    imags = [by_real[:, j + 128 : j + 256] + by_imag[:, j : j + 128] for j in (0, 256)]
    return reals, imags


def along_t(blocks, table_ref):
    rows = blocks[0][0].shape[0]
    split_blocks = [[pieces(block) for block in part] for part in blocks]

    def pairs(k):
        return jnp.concatenate(
            [
                jnp.concatenate([split_blocks[p][g][k], split_blocks[p][(g + 1) % 4][k]], axis=1)
                for g in range(4)
                for p in range(2)
            ],
            axis=0,
        )

    high, low = pairs(0), pairs(1)
    r = dot(high, table_ref[0]) + (dot(low, table_ref[0]) + dot(high, table_ref[1]))

    def product(g, p):
        upper = (2 * g + p) * rows
        lower = (2 * ((g + 2) % 4) + p) * rows
        return r[upper : upper + rows, :256] + r[lower : lower + rows, 256:]

    outs = [[], []]
    for g in range(4):
        from_real = product(g, 0)
        from_imag = product(g, 1)
        outs[0].append(from_real[:, :128] - from_imag[:, 128:])
        outs[1].append(from_imag[:, :128] + from_real[:, 128:])
    return outs


def turns(angle):
    count = jnp.floor(angle * (2.0 / math.pi) + 0.5)
    rest = ((angle - count * 1.5703125) - count * 4.837512969970703125e-4) - count * 7.54978995489188216e-8
    quadrant = count.astype(jnp.int32)
    square = rest * rest
    sine = rest + rest * square * (-1.6666654611e-1 + square * (8.3321608736e-3 - 1.9515295891e-4 * square))
    cosine = (1.0 - 0.5 * square) + square * square * (
        4.166664568298827e-2 + square * (-1.388731625493765e-3 + 2.443315711809948e-5 * square)
    )
    odd = (quadrant & 1) == 1
    cos_turn = jnp.where(odd, sine, cosine)
    sin_turn = jnp.where(odd, cosine, sine)
    return (
        jnp.where(((quadrant + 1) & 2) == 2, -cos_turn, cos_turn),
        jnp.where((quadrant & 2) == 2, -sin_turn, sin_turn),
    )


def first_kernel(field_hbm, table_hbm, out_ref, field_ref, table_ref, sems):
    copies = []
    for p in range(2):
        copies.append(pltpu.make_async_copy(field_hbm.at[p], field_ref.at[p], sems.at[2 * p]))
        copies.append(pltpu.make_async_copy(table_hbm.at[p], table_ref.at[p], sems.at[2 * p + 1]))
    for copy in copies:
        copy.start()
    for copy in copies:
        copy.wait()
    real = field_ref[0]
    imag = field_ref[1]
    reals, imags = along_y(real, imag, table_ref)
    half = NY // 2
    for j in range(2):
        out_ref[pl.ds(3 * half * j, half, stride=3), :] = reals[j]
        out_ref[pl.ds(3 * half * j + 1, half, stride=3), :] = imags[j]
    power = jnp.sum(real * real + imag * imag, axis=0, keepdims=True)
    out_ref[pl.ds(2, NY, stride=3), :] = jnp.broadcast_to(power, (NY, 128))


def time_kernel(in_ref, table_ref, out_ref):
    blocks = [[in_ref[pl.ds(3 * g + p, HALF_X, stride=12), :] for g in range(4)] for p in range(2)]
    outs = along_t(blocks, table_ref)
    for p in range(2):
        for g in range(4):
            out_ref[p * HALF_X : (p + 1) * HALF_X, 128 * g : 128 * (g + 1)] = outs[p][g]
    power = jnp.sum(in_ref[pl.ds(2, NY, stride=3), :], axis=0, keepdims=True)
    out_ref[NX:, :128] = jnp.broadcast_to(power, (8, 128))


def kick_kernel(mine_ref, other_ref, x_table_ref, t_table_ref, out_ref):
    core = lax.axis_index("c")
    place_y = ((lax.axis_index(CHIPS) ^ FLIP).astype(jnp.float32) - (NY - 1) / 2.0) / (NY / 2.0)
    well_y = WELL * place_y * place_y
    total = jnp.sum(mine_ref[NX : NX + 1, :128] + other_ref[NX : NX + 1, :128], axis=1, keepdims=True)
    scale = 1.0 / jnp.sqrt(total * (1.0 / (NX * NY * NT)) + EPSILON)
    table = x_table_ref[0, core]
    table_low = x_table_ref[1, core]
    own, own_low = [jnp.concatenate([t[:HALF_X], t[NX : NX + HALF_X]], axis=0) for t in (table, table_low)]
    width = NT // 2
    row = lax.broadcasted_iota(jnp.int32, (8, width), 0)

    def along_x(b):
        parts = [
            ref[p * HALF_X : (p + 1) * HALF_X, b * width : (b + 1) * width]
            for p in range(2)
            for ref in (mine_ref, other_ref)
        ]
        high, low = pieces(jnp.concatenate(parts, axis=0))
        return dot(table, high) + (dot(table, low) + dot(table_low, high))

    def kick(first):
        reals = []
        imags = []
        for start in range(0, NX, 8):
            parity = core if start < HALF_X else 1 - core
            x = 2 * ((start % HALF_X + row) ^ FLIP_X) + parity
            place_x = (x.astype(jnp.float32) - (NX - 1) / 2.0) / (NX / 2.0)
            real = first[start : start + 8] * scale
            imag = first[NX + start : NX + start + 8] * scale
            cos_turn, sin_turn = turns(KERR * (real * real + imag * imag) - (WELL * place_x * place_x + well_y))
            reals.append(real * cos_turn - imag * sin_turn)
            imags.append(real * sin_turn + imag * cos_turn)
        return jnp.concatenate(reals + imags, axis=0)

    def along_x_own(kicked):
        high, low = pieces(kicked)
        return dot(own, high) + (dot(own, low) + dot(own_low, high))

    firsts = [along_x(0), along_x(1)]
    seconds = [along_x_own(kick(first)) for first in firsts]
    blocks = [
        [seconds[g // 2][p * HALF_X : (p + 1) * HALF_X, 128 * (g % 2) : 128 * (g % 2 + 1)] for g in range(4)]
        for p in range(2)
    ]
    outs = along_t(blocks, t_table_ref)
    for p in range(2):
        for g in range(4):
            out_ref[pl.ds(2 * g + p, HALF_X, stride=8), :] = outs[p][g]


def last_kernel(in_ref, table_ref, out_ref):
    real = in_ref[pl.ds(0, NY, stride=2), :]
    imag = in_ref[pl.ds(1, NY, stride=2), :]
    reals, imags = along_y(real, imag, table_ref)
    half = NY // 2
    for j in range(2):
        out_ref[0, j * half : (j + 1) * half] = reals[j]
        out_ref[1, j * half : (j + 1) * half] = imags[j]


def call(kernel, shape, *args, scratch=(), direct=False):
    source = pltpu.HBM if direct else pltpu.VMEM
    return pl.pallas_call(
        kernel,
        in_specs=[pl.BlockSpec(memory_space=source) for _ in args],
        out_specs=pl.BlockSpec(memory_space=pltpu.VMEM),
        out_shape=jax.ShapeDtypeStruct(shape, jnp.float32),
        scratch_shapes=list(scratch),
        compiler_params=pltpu.CompilerParams(vmem_limit_bytes=16 * 2**20),
        name=kernel.__name__,
    )(*args)


def groups():
    chips = [position ^ FLIP for position in range(NY)]
    return [[(chip >> 2) * 8 + core * 4 + (chip & 3) for chip in chips] for core in range(2)]


def to_chips(rows, count):
    moved = lax.all_to_all(
        rows.reshape(NY, 1, count * 128),
        DEVICES,
        split_axis=0,
        concat_axis=0,
        tiled=True,
        axis_index_groups=groups(),
    )
    return moved.reshape(count * NY, 128)


def on_device(field, y_table, t_table, x_table):
    scratch = [pltpu.VMEM((2, NY, 128), jnp.float32), pltpu.VMEM(y_table.shape, jnp.bfloat16), pltpu.SemaphoreType.DMA((4,))]
    from_hbm = [pltpu.with_memory_space_constraint(a, pltpu.HBM) for a in (field.reshape(2, NY, 128), y_table)]
    rows = call(first_kernel, (3 * NY, 128), *from_hbm, scratch=scratch, direct=True)
    mine = call(time_kernel, (NX + 8, NT), to_chips(rows, 3), t_table)
    other = lax.ppermute(mine, "c", [(0, 1), (1, 0)])
    rows = call(kick_kernel, (2 * NY, 128), mine, other, x_table, t_table)
    out = call(last_kernel, (2, NY, 128), to_chips(rows, 2), y_table)
    return out.reshape(2, 1, NY, 128)


def solution(mesh):
    torus = Mesh(mesh.devices.reshape(8, 4, 2, 2, mesh.shape["tm"]), DEVICES)
    along_x = propagator(NX, -DIFFRACT)
    runs = np.arange(HALF_X) ^ FLIP_X
    x_tables = []
    for core in range(2):
        order = np.concatenate([2 * runs + core, 2 * runs + 1 - core])
        x_tables.append(real_block(along_x[order][:, order]))
    y_rows = propagator(NY, -DIFFRACT)[: NY // 2]
    t_columns = propagator(NT, DISPERSE).T[:, :128]
    t_columns = np.concatenate([t_columns.real, t_columns.imag], axis=1)
    tables = (
        split(np.concatenate([y_rows.real, y_rows.imag], axis=0)),
        split(np.concatenate([t_columns[: NT // 2], t_columns[NT // 2 :]], axis=1)),
        np.stack(x_tables, axis=1),
    )
    placed = P(None, SLAB, None, "t")
    inner = jax.shard_map(
        lambda field: on_device(field, *[jnp.asarray(table) for table in tables]),
        mesh=torus,
        in_specs=(placed,),
        out_specs=placed,
        check_vma=False,
    )
    return inner
```

```python
import math

import jax
import jax.numpy as jnp
import ml_dtypes
import numpy as np
from jax import lax
from jax.experimental import pallas as pl
from jax.experimental.pallas import tpu as pltpu
from jax.sharding import Mesh
from jax.sharding import PartitionSpec as P

NX = 128
NY = 256
NT = 512
HALF_X = NX // 2
SLAB = ("z", "x", "h", "c")
DEVICES = ("z", "x", "h", "c", "t")
RUN_BITS = (5, 4, 3, 2, 1, 0)
FLIP = 37
T_HIGH = True

TWO_PI = 2.0 * math.pi
DIFFRACT = 4.0
DISPERSE = 3.0
KERR = 0.05
WELL = 1.5
EPSILON = 1e-06


def propagator(length, weight):
    positions = np.arange(length)
    signed = np.where(2 * positions < length, positions, positions - length)
    angle = weight * (signed * (TWO_PI / length)) ** 2
    kernel = np.fft.ifft(np.exp(1j * angle))
    return kernel[(positions[:, None] - positions[None, :]) % length]


def split(matrix):
    full = matrix.astype(np.float32)
    high = full.astype(ml_dtypes.bfloat16)
    low = (matrix - high.astype(np.float64)).astype(ml_dtypes.bfloat16)
    return np.stack([high, low])


def spread(place):
    return sum(((place >> i) & 1) << bit for i, bit in enumerate(RUN_BITS))


def run_at(place):
    return spread(place) ^ FLIP


def position_of(run, t):
    place = sum((((run ^ FLIP) >> bit) & 1) << i for i, bit in enumerate(RUN_BITS))
    return t * HALF_X + place if T_HIGH else 4 * place + t


def rows_of(t, part, count):
    if T_HIGH:
        return pl.ds(count * HALF_X * t + part, HALF_X, stride=count)
    return pl.ds(count * t + part, HALF_X, stride=4 * count)


def real_block(matrix):
    return split(np.block([[matrix.real, -matrix.imag], [matrix.imag, matrix.real]]))


def pieces(value):
    high = value.astype(jnp.bfloat16)
    return high, (value - high.astype(jnp.float32)).astype(jnp.bfloat16)


def dot(left, right):
    return jnp.dot(left, right, preferred_element_type=jnp.float32)


def along_y(real, imag, table_ref):
    straight = jnp.concatenate([real, imag], axis=1)
    half = NY // 2
    data = jnp.concatenate([straight, jnp.concatenate([straight[half:], straight[:half]], axis=0)], axis=1)
    high, low = pieces(data)
    r = dot(table_ref[0], high) + (dot(table_ref[0], low) + dot(table_ref[1], high))
    by_real = r[:half]
    by_imag = r[half:]
    reals = [by_real[:, j : j + 128] - by_imag[:, j + 128 : j + 256] for j in (0, 256)]
    imags = [by_real[:, j + 128 : j + 256] + by_imag[:, j : j + 128] for j in (0, 256)]
    return reals, imags


def along_t(blocks, table_ref):
    rows = blocks[0][0].shape[0]
    split_blocks = [[pieces(block) for block in part] for part in blocks]

    def pairs(k):
        return jnp.concatenate(
            [
                jnp.concatenate([split_blocks[p][g][k], split_blocks[p][(g + 1) % 4][k]], axis=1)
                for g in range(4)
                for p in range(2)
            ],
            axis=0,
        )

    high, low = pairs(0), pairs(1)
    r = dot(high, table_ref[0]) + (dot(low, table_ref[0]) + dot(high, table_ref[1]))

    def product(g, p):
        upper = (2 * g + p) * rows
        lower = (2 * ((g + 2) % 4) + p) * rows
        return r[upper : upper + rows, :256] + r[lower : lower + rows, 256:]

    outs = [[], []]
    for g in range(4):
        from_real = product(g, 0)
        from_imag = product(g, 1)
        outs[0].append(from_real[:, :128] - from_imag[:, 128:])
        outs[1].append(from_imag[:, :128] + from_real[:, 128:])
    return outs


def turns(angle):
    count = jnp.floor(angle * (2.0 / math.pi) + 0.5)
    rest = ((angle - count * 1.5703125) - count * 4.837512969970703125e-4) - count * 7.54978995489188216e-8
    quadrant = count.astype(jnp.int32)
    square = rest * rest
    sine = rest + rest * square * (-1.6666654611e-1 + square * (8.3321608736e-3 - 1.9515295891e-4 * square))
    cosine = (1.0 - 0.5 * square) + square * square * (
        4.166664568298827e-2 + square * (-1.388731625493765e-3 + 2.443315711809948e-5 * square)
    )
    odd = (quadrant & 1) == 1
    cos_turn = jnp.where(odd, sine, cosine)
    sin_turn = jnp.where(odd, cosine, sine)
    return (
        jnp.where(((quadrant + 1) & 2) == 2, -cos_turn, cos_turn),
        jnp.where((quadrant & 2) == 2, -sin_turn, sin_turn),
    )


def first_kernel(field_hbm, table_hbm, out_ref, field_ref, table_ref, sems):
    copies = [
        pltpu.make_async_copy(field_hbm, field_ref, sems.at[0]),
        pltpu.make_async_copy(table_hbm, table_ref, sems.at[1]),
    ]
    for copy in copies:
        copy.start()
    for copy in copies:
        copy.wait()
    real = field_ref[0]
    imag = field_ref[1]
    reals, imags = along_y(real, imag, table_ref)
    half = NY // 2
    for j in range(2):
        out_ref[pl.ds(3 * half * j, half, stride=3), :] = reals[j]
        out_ref[pl.ds(3 * half * j + 1, half, stride=3), :] = imags[j]
    power = jnp.sum(real * real + imag * imag, axis=0, keepdims=True)
    out_ref[pl.ds(2, NY, stride=3), :] = jnp.broadcast_to(power, (NY, 128))


def time_kernel(in_ref, table_ref, out_ref):
    blocks = [[in_ref[rows_of(g, p, 3), :] for g in range(4)] for p in range(2)]
    outs = along_t(blocks, table_ref)
    for p in range(2):
        for g in range(4):
            out_ref[p * HALF_X : (p + 1) * HALF_X, 128 * g : 128 * (g + 1)] = outs[p][g]
    power = jnp.sum(in_ref[pl.ds(2, NY, stride=3), :], axis=0, keepdims=True)
    out_ref[NX:, :128] = jnp.broadcast_to(power, (8, 128))


def kick_kernel(mine_ref, other_ref, x_table_ref, t_table_ref, out_ref):
    core = lax.axis_index("c")
    position = position_of(lax.axis_index(("z", "x", "h")), lax.axis_index("t"))
    place_y = (position.astype(jnp.float32) - (NY - 1) / 2.0) / (NY / 2.0)
    well_y = WELL * place_y * place_y
    total = jnp.sum(mine_ref[NX : NX + 1, :128] + other_ref[NX : NX + 1, :128], axis=1, keepdims=True)
    scale = 1.0 / jnp.sqrt(total * (1.0 / (NX * NY * NT)) + EPSILON)
    table = x_table_ref[0, core]
    table_low = x_table_ref[1, core]
    own, own_low = [jnp.concatenate([t[:HALF_X], t[NX : NX + HALF_X]], axis=0) for t in (table, table_low)]
    width = NT // 2
    low_run = spread(lax.broadcasted_iota(jnp.int32, (8, width), 0))

    def along_x(b):
        parts = [
            ref[p * HALF_X : (p + 1) * HALF_X, b * width : (b + 1) * width]
            for p in range(2)
            for ref in (mine_ref, other_ref)
        ]
        high, low = pieces(jnp.concatenate(parts, axis=0))
        return dot(table, high) + (dot(table, low) + dot(table_low, high))

    def kick(first):
        reals = []
        imags = []
        for start in range(0, NX, 8):
            parity = core if start < HALF_X else 1 - core
            x = 2 * (low_run ^ run_at(start % HALF_X)) + parity
            place_x = (x.astype(jnp.float32) - (NX - 1) / 2.0) / (NX / 2.0)
            real = first[start : start + 8] * scale
            imag = first[NX + start : NX + start + 8] * scale
            cos_turn, sin_turn = turns(KERR * (real * real + imag * imag) - (WELL * place_x * place_x + well_y))
            reals.append(real * cos_turn - imag * sin_turn)
            imags.append(real * sin_turn + imag * cos_turn)
        return jnp.concatenate(reals + imags, axis=0)

    def along_x_own(kicked):
        high, low = pieces(kicked)
        return dot(own, high) + (dot(own, low) + dot(own_low, high))

    firsts = [along_x(0), along_x(1)]
    seconds = [along_x_own(kick(first)) for first in firsts]
    blocks = [
        [seconds[g // 2][p * HALF_X : (p + 1) * HALF_X, 128 * (g % 2) : 128 * (g % 2 + 1)] for g in range(4)]
        for p in range(2)
    ]
    outs = along_t(blocks, t_table_ref)
    for p in range(2):
        for g in range(4):
            out_ref[rows_of(g, p, 2), :] = outs[p][g]


def last_kernel(in_ref, table_ref, out_ref):
    real = in_ref[pl.ds(0, NY, stride=2), :]
    imag = in_ref[pl.ds(1, NY, stride=2), :]
    reals, imags = along_y(real, imag, table_ref)
    half = NY // 2
    for j in range(2):
        out_ref[0, j * half : (j + 1) * half] = reals[j]
        out_ref[1, j * half : (j + 1) * half] = imags[j]


def call(kernel, shape, *args, scratch=(), direct=False):
    source = pltpu.HBM if direct else pltpu.VMEM
    return pl.pallas_call(
        kernel,
        in_specs=[pl.BlockSpec(memory_space=source) for _ in args],
        out_specs=pl.BlockSpec(memory_space=pltpu.VMEM),
        out_shape=jax.ShapeDtypeStruct(shape, jnp.float32),
        scratch_shapes=list(scratch),
        compiler_params=pltpu.CompilerParams(vmem_limit_bytes=16 * 2**20),
        name=kernel.__name__,
    )(*args)


def groups():
    found = np.empty((2, NY), np.int64)
    for run in range(HALF_X):
        for t in range(4):
            for core in range(2):
                found[core, position_of(run, t)] = run * 8 + core * 4 + t
    return found.tolist()


def to_chips(rows, count):
    moved = lax.all_to_all(
        rows.reshape(NY, 1, count * 128),
        DEVICES,
        split_axis=0,
        concat_axis=0,
        tiled=True,
        axis_index_groups=groups(),
    )
    return moved.reshape(count * NY, 128)


def on_device(field, y_table, t_table, x_table):
    scratch = [pltpu.VMEM((2, NY, 128), jnp.float32), pltpu.VMEM(y_table.shape, jnp.bfloat16), pltpu.SemaphoreType.DMA((2,))]
    from_hbm = [pltpu.with_memory_space_constraint(a, pltpu.HBM) for a in (field.reshape(2, NY, 128), y_table)]
    rows = call(first_kernel, (3 * NY, 128), *from_hbm, scratch=scratch, direct=True)
    mine = call(time_kernel, (NX + 8, NT), to_chips(rows, 3), t_table)
    other = lax.ppermute(mine, "c", [(0, 1), (1, 0)])
    rows = call(kick_kernel, (2 * NY, 128), mine, other, x_table, t_table)
    out = call(last_kernel, (2, NY, 128), to_chips(rows, 2), y_table)
    return out.reshape(2, 1, NY, 128)


def solution(mesh):
    torus = Mesh(mesh.devices.reshape(8, 4, 2, 2, mesh.shape["tm"]), DEVICES)
    along_x = propagator(NX, -DIFFRACT)
    runs = run_at(np.arange(HALF_X))
    x_tables = []
    for core in range(2):
        order = np.concatenate([2 * runs + core, 2 * runs + 1 - core])
        x_tables.append(real_block(along_x[order][:, order]))
    y_rows = propagator(NY, -DIFFRACT)[: NY // 2]
    t_columns = propagator(NT, DISPERSE).T[:, :128]
    t_columns = np.concatenate([t_columns.real, t_columns.imag], axis=1)
    tables = (
        split(np.concatenate([y_rows.real, y_rows.imag], axis=0)),
        split(np.concatenate([t_columns[: NT // 2], t_columns[NT // 2 :]], axis=1)),
        np.stack(x_tables, axis=1),
    )
    placed = P(None, SLAB, None, "t")
    inner = jax.shard_map(
        lambda field: on_device(field, *[jnp.asarray(table) for table in tables]),
        mesh=torus,
        in_specs=(placed,),
        out_specs=placed,
        check_vma=False,
    )
    return inner
```

```python
import math

import jax
import jax.numpy as jnp
import ml_dtypes
import numpy as np
from jax import lax
from jax.experimental import pallas as pl
from jax.experimental.pallas import tpu as pltpu
from jax.sharding import Mesh
from jax.sharding import PartitionSpec as P

NX = 128
NY = 256
NT = 512
HALF_X = NX // 2
SLAB = ("z", "x", "h", "c")
DEVICES = ("z", "x", "h", "c", "t")
RUN_BITS = (5, 4, 3, 2, 1, 0)
FLIP = 37
T_HIGH = True

TWO_PI = 2.0 * math.pi
DIFFRACT = 4.0
DISPERSE = 3.0
KERR = 0.05
WELL = 1.5
EPSILON = 1e-06


def propagator(length, weight):
    positions = np.arange(length)
    signed = np.where(2 * positions < length, positions, positions - length)
    angle = weight * (signed * (TWO_PI / length)) ** 2
    kernel = np.fft.ifft(np.exp(1j * angle))
    return kernel[(positions[:, None] - positions[None, :]) % length]


def split(matrix):
    full = matrix.astype(np.float32)
    high = full.astype(ml_dtypes.bfloat16)
    low = (matrix - high.astype(np.float64)).astype(ml_dtypes.bfloat16)
    return np.stack([high, low])


def spread(place):
    return sum(((place >> i) & 1) << bit for i, bit in enumerate(RUN_BITS))


def run_at(place):
    return spread(place) ^ FLIP


def position_of(run, t):
    place = sum((((run ^ FLIP) >> bit) & 1) << i for i, bit in enumerate(RUN_BITS))
    return t * HALF_X + place if T_HIGH else 4 * place + t


def rows_of(t, part, count):
    if T_HIGH:
        return pl.ds(count * HALF_X * t + part, HALF_X, stride=count)
    return pl.ds(count * t + part, HALF_X, stride=4 * count)


def real_block(matrix):
    return split(np.block([[matrix.real, -matrix.imag], [matrix.imag, matrix.real]]))


def pieces(value):
    high = value.astype(jnp.bfloat16)
    return high, (value - high.astype(jnp.float32)).astype(jnp.bfloat16)


def dot(left, right):
    return jnp.dot(left, right, preferred_element_type=jnp.float32)


def along_y(real, imag, table_ref):
    straight = jnp.concatenate([real, imag], axis=1)
    half = NY // 2
    data = jnp.concatenate([straight, jnp.concatenate([straight[half:], straight[:half]], axis=0)], axis=1)
    high, low = pieces(data)
    r = dot(table_ref[0], high) + (dot(table_ref[0], low) + dot(table_ref[1], high))
    by_real = r[:half]
    by_imag = r[half:]
    reals = [by_real[:, j : j + 128] - by_imag[:, j + 128 : j + 256] for j in (0, 256)]
    imags = [by_real[:, j + 128 : j + 256] + by_imag[:, j : j + 128] for j in (0, 256)]
    return reals, imags


def along_t(blocks, table_ref):
    rows = blocks[0][0].shape[0]
    split_blocks = [[pieces(block) for block in part] for part in blocks]

    def pairs(k):
        return jnp.concatenate(
            [
                jnp.concatenate([split_blocks[p][g][k], split_blocks[p][(g + 1) % 4][k]], axis=1)
                for g in range(4)
                for p in range(2)
            ],
            axis=0,
        )

    high, low = pairs(0), pairs(1)
    r = dot(high, table_ref[0]) + (dot(low, table_ref[0]) + dot(high, table_ref[1]))

    def product(g, p):
        upper = (2 * g + p) * rows
        lower = (2 * ((g + 2) % 4) + p) * rows
        return r[upper : upper + rows, :256] + r[lower : lower + rows, 256:]

    outs = [[], []]
    for g in range(4):
        from_real = product(g, 0)
        from_imag = product(g, 1)
        outs[0].append(from_real[:, :128] - from_imag[:, 128:])
        outs[1].append(from_imag[:, :128] + from_real[:, 128:])
    return outs


def turns(half):
    count = jnp.floor(half * (1.0 / math.pi) + 0.5)
    rest = ((half - count * 3.140625) - count * 9.67502593994140625e-4) - count * 1.509957990978376432e-7
    square = rest * rest
    sine = rest + (rest * square) * (
        -1.66666563e-1 + square * (8.33299813e-3 + square * (-1.98052344e-4 + square * 2.59701156e-6))
    )
    cosine = 1.0 + square * (
        -4.99999268e-1 + square * (4.16638274e-2 + square * (-1.38546172e-3 + square * 2.31630858e-5))
    )
    twice = sine + sine
    return 1.0 - twice * sine, twice * cosine


def first_kernel(field_hbm, table_hbm, out_ref, field_ref, table_ref, sems):
    copies = [
        pltpu.make_async_copy(field_hbm, field_ref, sems.at[0]),
        pltpu.make_async_copy(table_hbm, table_ref, sems.at[1]),
    ]
    for copy in copies:
        copy.start()
    for copy in copies:
        copy.wait()
    real = field_ref[0]
    imag = field_ref[1]
    reals, imags = along_y(real, imag, table_ref)
    half = NY // 2
    for j in range(2):
        out_ref[pl.ds(3 * half * j, half, stride=3), :] = reals[j]
        out_ref[pl.ds(3 * half * j + 1, half, stride=3), :] = imags[j]
    power = jnp.sum(real * real + imag * imag, axis=0, keepdims=True)
    out_ref[pl.ds(2, NY, stride=3), :] = jnp.broadcast_to(power, (NY, 128))


def time_kernel(in_ref, table_ref, out_ref):
    blocks = [[in_ref[rows_of(g, p, 3), :] for g in range(4)] for p in range(2)]
    outs = along_t(blocks, table_ref)
    for p in range(2):
        for g in range(4):
            out_ref[p * HALF_X : (p + 1) * HALF_X, 128 * g : 128 * (g + 1)] = outs[p][g]
    power = jnp.sum(in_ref[pl.ds(2, NY, stride=3), :], axis=0, keepdims=True)
    out_ref[NX:, :128] = jnp.broadcast_to(power, (8, 128))


def kick_kernel(mine_ref, other_ref, x_table_ref, t_table_ref, out_ref):
    core = lax.axis_index("c")
    position = position_of(lax.axis_index(("z", "x", "h")), lax.axis_index("t"))
    place_y = (position.astype(jnp.float32) - (NY - 1) / 2.0) / (NY / 2.0)
    total = jnp.sum(mine_ref[NX : NX + 1, :128] + other_ref[NX : NX + 1, :128], axis=1, keepdims=True)
    scale = 1.0 / jnp.sqrt(total * (1.0 / (NX * NY * NT)) + EPSILON)
    table = x_table_ref[0, core]
    table_low = x_table_ref[1, core]
    own, own_low = [jnp.concatenate([t[:HALF_X], t[NX : NX + HALF_X]], axis=0) for t in (table, table_low)]
    width = NT // 2
    half_kerr = (0.5 * KERR) * scale * scale
    low_run = spread(lax.broadcasted_iota(jnp.int32, (8, 128), 0))
    half_wells = []
    for start in range(0, NX, 8):
        x = 2 * (low_run ^ run_at(start % HALF_X)) + (core if start < HALF_X else 1 - core)
        place_x = (x.astype(jnp.float32) - (NX - 1) / 2.0) / (NX / 2.0)
        half_well = (0.5 * WELL) * (place_x * place_x + place_y * place_y)
        half_wells.append(jnp.concatenate([half_well] * (width // 128), axis=1))

    def along_x(b):
        parts = [
            ref[p * HALF_X : (p + 1) * HALF_X, b * width : (b + 1) * width]
            for p in range(2)
            for ref in (mine_ref, other_ref)
        ]
        high, low = pieces(jnp.concatenate(parts, axis=0))
        return dot(table, high) + (dot(table, low) + dot(table_low, high))

    def kick(first):
        reals = []
        imags = []
        for start in range(0, NX, 8):
            real = first[start : start + 8]
            imag = first[NX + start : NX + start + 8]
            cos_turn, sin_turn = turns(half_kerr * (real * real + imag * imag) - half_wells[start // 8])
            reals.append(real * cos_turn - imag * sin_turn)
            imags.append(real * sin_turn + imag * cos_turn)
        return jnp.concatenate(reals + imags, axis=0)

    def along_x_own(kicked):
        high, low = pieces(kicked)
        return dot(own, high) + (dot(own, low) + dot(own_low, high))

    firsts = [along_x(0), along_x(1)]
    seconds = [along_x_own(kick(first)) for first in firsts]
    blocks = [
        [seconds[g // 2][p * HALF_X : (p + 1) * HALF_X, 128 * (g % 2) : 128 * (g % 2 + 1)] for g in range(4)]
        for p in range(2)
    ]
    outs = along_t(blocks, t_table_ref)
    for p in range(2):
        for g in range(4):
            out_ref[rows_of(g, p, 2), :] = outs[p][g] * scale


def last_kernel(in_ref, table_ref, out_ref):
    real = in_ref[pl.ds(0, NY, stride=2), :]
    imag = in_ref[pl.ds(1, NY, stride=2), :]
    reals, imags = along_y(real, imag, table_ref)
    half = NY // 2
    for j in range(2):
        out_ref[0, j * half : (j + 1) * half] = reals[j]
        out_ref[1, j * half : (j + 1) * half] = imags[j]


def call(kernel, shape, *args, scratch=(), direct=False):
    source = pltpu.HBM if direct else pltpu.VMEM
    return pl.pallas_call(
        kernel,
        in_specs=[pl.BlockSpec(memory_space=source) for _ in args],
        out_specs=pl.BlockSpec(memory_space=pltpu.VMEM),
        out_shape=jax.ShapeDtypeStruct(shape, jnp.float32),
        scratch_shapes=list(scratch),
        compiler_params=pltpu.CompilerParams(vmem_limit_bytes=16 * 2**20),
        name=kernel.__name__,
    )(*args)


def groups():
    found = np.empty((2, NY), np.int64)
    for run in range(HALF_X):
        for t in range(4):
            for core in range(2):
                found[core, position_of(run, t)] = run * 8 + core * 4 + t
    return found.tolist()


def to_chips(rows, count):
    moved = lax.all_to_all(
        rows.reshape(NY, 1, count * 128),
        DEVICES,
        split_axis=0,
        concat_axis=0,
        tiled=True,
        axis_index_groups=groups(),
    )
    return moved.reshape(count * NY, 128)


def on_device(field, y_table, t_table, x_table):
    scratch = [pltpu.VMEM((2, NY, 128), jnp.float32), pltpu.VMEM(y_table.shape, jnp.bfloat16), pltpu.SemaphoreType.DMA((2,))]
    from_hbm = [pltpu.with_memory_space_constraint(a, pltpu.HBM) for a in (field.reshape(2, NY, 128), y_table)]
    rows = call(first_kernel, (3 * NY, 128), *from_hbm, scratch=scratch, direct=True)
    mine = call(time_kernel, (NX + 8, NT), to_chips(rows, 3), t_table)
    other = lax.ppermute(mine, "c", [(0, 1), (1, 0)])
    rows = call(kick_kernel, (2 * NY, 128), mine, other, x_table, t_table)
    out = call(last_kernel, (2, NY, 128), to_chips(rows, 2), y_table)
    return out.reshape(2, 1, NY, 128)


def solution(mesh):
    torus = Mesh(mesh.devices.reshape(8, 4, 2, 2, mesh.shape["tm"]), DEVICES)
    along_x = propagator(NX, -DIFFRACT)
    runs = run_at(np.arange(HALF_X))
    x_tables = []
    for core in range(2):
        order = np.concatenate([2 * runs + core, 2 * runs + 1 - core])
        x_tables.append(real_block(along_x[order][:, order]))
    y_rows = propagator(NY, -DIFFRACT)[: NY // 2]
    t_columns = propagator(NT, DISPERSE).T[:, :128]
    t_columns = np.concatenate([t_columns.real, t_columns.imag], axis=1)
    tables = (
        split(np.concatenate([y_rows.real, y_rows.imag], axis=0)),
        split(np.concatenate([t_columns[: NT // 2], t_columns[NT // 2 :]], axis=1)),
        np.stack(x_tables, axis=1),
    )
    placed = P(None, SLAB, None, "t")
    inner = jax.shard_map(
        lambda field: on_device(field, *[jnp.asarray(table) for table in tables]),
        mesh=torus,
        in_specs=(placed,),
        out_specs=placed,
        check_vma=False,
    )
    return inner
```

```python
import math

import jax
import jax.numpy as jnp
import ml_dtypes
import numpy as np
from jax import lax
from jax.experimental import pallas as pl
from jax.experimental.pallas import tpu as pltpu
from jax.sharding import Mesh
from jax.sharding import PartitionSpec as P

NX = 128
NY = 256
NT = 512
HALF_X = NX // 2
SLAB = ("z", "x", "h", "c")
DEVICES = ("z", "x", "h", "c", "t")
RUN_BITS = (5, 4, 3, 2, 1, 0)
FLIP = 37
T_HIGH = True

TWO_PI = 2.0 * math.pi
DIFFRACT = 4.0
DISPERSE = 3.0
KERR = 0.05
WELL = 1.5
EPSILON = 1e-06


def propagator(length, weight):
    positions = np.arange(length)
    signed = np.where(2 * positions < length, positions, positions - length)
    angle = weight * (signed * (TWO_PI / length)) ** 2
    kernel = np.fft.ifft(np.exp(1j * angle))
    return kernel[(positions[:, None] - positions[None, :]) % length]


def split(matrix):
    full = matrix.astype(np.float32)
    high = full.astype(ml_dtypes.bfloat16)
    low = (matrix - high.astype(np.float64)).astype(ml_dtypes.bfloat16)
    return np.stack([high, low])


def spread(place):
    return sum(((place >> i) & 1) << bit for i, bit in enumerate(RUN_BITS))


def run_at(place):
    return spread(place) ^ FLIP


def position_of(run, t):
    place = sum((((run ^ FLIP) >> bit) & 1) << i for i, bit in enumerate(RUN_BITS))
    return t * HALF_X + place if T_HIGH else 4 * place + t


def rows_of(t, part, count):
    if T_HIGH:
        return pl.ds(count * HALF_X * t + part, HALF_X, stride=count)
    return pl.ds(count * t + part, HALF_X, stride=4 * count)


def real_block(matrix):
    return split(np.block([[matrix.real, -matrix.imag], [matrix.imag, matrix.real]]))


def pieces(value):
    high = value.astype(jnp.bfloat16)
    return high, (value - high.astype(jnp.float32)).astype(jnp.bfloat16)


def dot(left, right):
    return jnp.dot(left, right, preferred_element_type=jnp.float32)


def along_y(real, imag, table_ref):
    straight = jnp.concatenate([real, imag], axis=1)
    half = NY // 2
    data = jnp.concatenate([straight, jnp.concatenate([straight[half:], straight[:half]], axis=0)], axis=1)
    high, low = pieces(data)
    r = dot(table_ref[0], high) + (dot(table_ref[0], low) + dot(table_ref[1], high))
    by_real = r[:half]
    by_imag = r[half:]
    reals = [by_real[:, j : j + 128] - by_imag[:, j + 128 : j + 256] for j in (0, 256)]
    imags = [by_real[:, j + 128 : j + 256] + by_imag[:, j : j + 128] for j in (0, 256)]
    return reals, imags


def along_t(blocks, table_ref):
    rows = blocks[0][0].shape[0]
    split_blocks = [[pieces(block) for block in part] for part in blocks]

    def pairs(k):
        return jnp.concatenate(
            [
                jnp.concatenate([split_blocks[p][g][k], split_blocks[p][(g + 1) % 4][k]], axis=1)
                for g in range(4)
                for p in range(2)
            ],
            axis=0,
        )

    high, low = pairs(0), pairs(1)
    r = dot(high, table_ref[0]) + (dot(low, table_ref[0]) + dot(high, table_ref[1]))

    def product(g, p):
        upper = (2 * g + p) * rows
        lower = (2 * ((g + 2) % 4) + p) * rows
        return r[upper : upper + rows, :256] + r[lower : lower + rows, 256:]

    outs = [[], []]
    for g in range(4):
        from_real = product(g, 0)
        from_imag = product(g, 1)
        outs[0].append(from_real[:, :128] - from_imag[:, 128:])
        outs[1].append(from_imag[:, :128] + from_real[:, 128:])
    return outs


def turns(half):
    count = jnp.floor(half * (1.0 / math.pi) + 0.5)
    rest = ((half - count * 3.140625) - count * 9.67502593994140625e-4) - count * 1.509957990978376432e-7
    square = rest * rest
    sine = rest + (rest * square) * (
        -1.66666563e-1 + square * (8.33299813e-3 + square * (-1.98052344e-4 + square * 2.59701156e-6))
    )
    cosine = 1.0 + square * (
        -4.99999268e-1 + square * (4.16638274e-2 + square * (-1.38546172e-3 + square * 2.31630858e-5))
    )
    twice = sine + sine
    return 1.0 - twice * sine, twice * cosine


def first_kernel(field_hbm, table_hbm, out_ref, field_ref, table_ref, sems):
    copies = [
        pltpu.make_async_copy(field_hbm, field_ref, sems.at[0]),
        pltpu.make_async_copy(table_hbm, table_ref, sems.at[1]),
    ]
    for copy in copies:
        copy.start()
    for copy in copies:
        copy.wait()
    real = field_ref[0]
    imag = field_ref[1]
    reals, imags = along_y(real, imag, table_ref)
    half = NY // 2
    for j in range(2):
        out_ref[pl.ds(3 * half * j, half, stride=3), :] = reals[j]
        out_ref[pl.ds(3 * half * j + 1, half, stride=3), :] = imags[j]
    power = jnp.sum(real * real + imag * imag, axis=0, keepdims=True)
    out_ref[pl.ds(2, NY, stride=3), :] = jnp.broadcast_to(power, (NY, 128))


def kick_kernel(mine_ref, other_ref, x_table_ref, t_table_ref, out_ref):
    core = lax.axis_index("c")
    position = position_of(lax.axis_index(("z", "x", "h")), lax.axis_index("t"))
    place_y = (position.astype(jnp.float32) - (NY - 1) / 2.0) / (NY / 2.0)
    powers = mine_ref[pl.ds(2, NY, stride=3), :] + other_ref[pl.ds(2, NY, stride=3), :]
    total = jnp.sum(jnp.sum(powers, axis=0, keepdims=True), axis=1, keepdims=True)
    scale = 1.0 / jnp.sqrt(total * (1.0 / (NX * NY * NT)) + EPSILON)
    table = x_table_ref[0, core]
    table_low = x_table_ref[1, core]
    own, own_low = [jnp.concatenate([t[:HALF_X], t[NX : NX + HALF_X]], axis=0) for t in (table, table_low)]
    width = NT // 2
    half_kerr = (0.5 * KERR) * scale * scale
    low_run = spread(lax.broadcasted_iota(jnp.int32, (8, 128), 0))
    half_wells = []
    for start in range(0, NX, 8):
        x = 2 * (low_run ^ run_at(start % HALF_X)) + (core if start < HALF_X else 1 - core)
        place_x = (x.astype(jnp.float32) - (NX - 1) / 2.0) / (NX / 2.0)
        half_well = (0.5 * WELL) * (place_x * place_x + place_y * place_y)
        half_wells.append(jnp.concatenate([half_well] * (width // 128), axis=1))

    turned = []
    for ref in (mine_ref, other_ref):
        blocks = [[ref[rows_of(g, p, 3), :] for g in range(4)] for p in range(2)]
        turned.append(along_t(blocks, t_table_ref))

    def along_x(b):
        parts = [
            jnp.concatenate(outs[p][2 * b : 2 * b + 2], axis=1)
            for p in range(2)
            for outs in turned
        ]
        high, low = pieces(jnp.concatenate(parts, axis=0))
        return dot(table, high) + (dot(table, low) + dot(table_low, high))

    def kick(first):
        reals = []
        imags = []
        for start in range(0, NX, 8):
            real = first[start : start + 8]
            imag = first[NX + start : NX + start + 8]
            cos_turn, sin_turn = turns(half_kerr * (real * real + imag * imag) - half_wells[start // 8])
            reals.append(real * cos_turn - imag * sin_turn)
            imags.append(real * sin_turn + imag * cos_turn)
        return jnp.concatenate(reals + imags, axis=0)

    def along_x_own(kicked):
        high, low = pieces(kicked)
        return dot(own, high) + (dot(own, low) + dot(own_low, high))

    firsts = [along_x(0), along_x(1)]
    seconds = [along_x_own(kick(first)) for first in firsts]
    blocks = [
        [seconds[g // 2][p * HALF_X : (p + 1) * HALF_X, 128 * (g % 2) : 128 * (g % 2 + 1)] for g in range(4)]
        for p in range(2)
    ]
    outs = along_t(blocks, t_table_ref)
    for p in range(2):
        for g in range(4):
            out_ref[rows_of(g, p, 2), :] = outs[p][g] * scale


def last_kernel(in_ref, table_ref, out_ref):
    real = in_ref[pl.ds(0, NY, stride=2), :]
    imag = in_ref[pl.ds(1, NY, stride=2), :]
    reals, imags = along_y(real, imag, table_ref)
    half = NY // 2
    for j in range(2):
        out_ref[0, j * half : (j + 1) * half] = reals[j]
        out_ref[1, j * half : (j + 1) * half] = imags[j]


def call(kernel, shape, *args, scratch=(), direct=False):
    source = pltpu.HBM if direct else pltpu.VMEM
    return pl.pallas_call(
        kernel,
        in_specs=[pl.BlockSpec(memory_space=source) for _ in args],
        out_specs=pl.BlockSpec(memory_space=pltpu.VMEM),
        out_shape=jax.ShapeDtypeStruct(shape, jnp.float32),
        scratch_shapes=list(scratch),
        compiler_params=pltpu.CompilerParams(vmem_limit_bytes=16 * 2**20),
        name=kernel.__name__,
    )(*args)


def groups():
    found = np.empty((2, NY), np.int64)
    for run in range(HALF_X):
        for t in range(4):
            for core in range(2):
                found[core, position_of(run, t)] = run * 8 + core * 4 + t
    return found.tolist()


def to_chips(rows, count):
    moved = lax.all_to_all(
        rows.reshape(NY, 1, count * 128),
        DEVICES,
        split_axis=0,
        concat_axis=0,
        tiled=True,
        axis_index_groups=groups(),
    )
    return moved.reshape(count * NY, 128)


def on_device(field, y_table, t_table, x_table):
    scratch = [pltpu.VMEM((2, NY, 128), jnp.float32), pltpu.VMEM(y_table.shape, jnp.bfloat16), pltpu.SemaphoreType.DMA((2,))]
    from_hbm = [pltpu.with_memory_space_constraint(a, pltpu.HBM) for a in (field.reshape(2, NY, 128), y_table)]
    rows = call(first_kernel, (3 * NY, 128), *from_hbm, scratch=scratch, direct=True)
    mine = to_chips(rows, 3)
    other = lax.ppermute(mine, "c", [(0, 1), (1, 0)])
    rows = call(kick_kernel, (2 * NY, 128), mine, other, x_table, t_table)
    out = call(last_kernel, (2, NY, 128), to_chips(rows, 2), y_table)
    return out.reshape(2, 1, NY, 128)


def solution(mesh):
    torus = Mesh(mesh.devices.reshape(8, 4, 2, 2, mesh.shape["tm"]), DEVICES)
    along_x = propagator(NX, -DIFFRACT)
    runs = run_at(np.arange(HALF_X))
    x_tables = []
    for core in range(2):
        order = np.concatenate([2 * runs + core, 2 * runs + 1 - core])
        x_tables.append(real_block(along_x[order][:, order]))
    y_rows = propagator(NY, -DIFFRACT)[: NY // 2]
    t_columns = propagator(NT, DISPERSE).T[:, :128]
    t_columns = np.concatenate([t_columns.real, t_columns.imag], axis=1)
    tables = (
        split(np.concatenate([y_rows.real, y_rows.imag], axis=0)),
        split(np.concatenate([t_columns[: NT // 2], t_columns[NT // 2 :]], axis=1)),
        np.stack(x_tables, axis=1),
    )
    placed = P(None, SLAB, None, "t")
    inner = jax.shard_map(
        lambda field: on_device(field, *[jnp.asarray(table) for table in tables]),
        mesh=torus,
        in_specs=(placed,),
        out_specs=placed,
        check_vma=False,
    )
    return inner
```

```python
import math

import jax
import jax.numpy as jnp
import ml_dtypes
import numpy as np
from jax import lax
from jax.experimental import pallas as pl
from jax.experimental.pallas import tpu as pltpu
from jax.sharding import Mesh
from jax.sharding import PartitionSpec as P

NX = 128
NY = 256
NT = 512
HALF_X = NX // 2
SLAB = ("z", "x", "h", "c")
DEVICES = ("z", "x", "h", "c", "t")
RUN_BITS = (5, 4, 3, 2, 1, 0)
FLIP = 37
T_HIGH = True

TWO_PI = 2.0 * math.pi
DIFFRACT = 4.0
DISPERSE = 3.0
KERR = 0.05
WELL = 1.5
EPSILON = 1e-06


def propagator(length, weight):
    positions = np.arange(length)
    signed = np.where(2 * positions < length, positions, positions - length)
    angle = weight * (signed * (TWO_PI / length)) ** 2
    kernel = np.fft.ifft(np.exp(1j * angle))
    return kernel[(positions[:, None] - positions[None, :]) % length]


def split(matrix):
    full = matrix.astype(np.float32)
    high = full.astype(ml_dtypes.bfloat16)
    low = (matrix - high.astype(np.float64)).astype(ml_dtypes.bfloat16)
    return np.stack([high, low])


def spread(place):
    return sum(((place >> i) & 1) << bit for i, bit in enumerate(RUN_BITS))


def run_at(place):
    return spread(place) ^ FLIP


def position_of(run, t):
    place = sum((((run ^ FLIP) >> bit) & 1) << i for i, bit in enumerate(RUN_BITS))
    return t * HALF_X + place if T_HIGH else 4 * place + t


def rows_of(t, part, count):
    if T_HIGH:
        return pl.ds(count * HALF_X * t + part, HALF_X, stride=count)
    return pl.ds(count * t + part, HALF_X, stride=4 * count)


def real_block(matrix):
    return split(np.block([[matrix.real, -matrix.imag], [matrix.imag, matrix.real]]))


def pieces(value):
    high = value.astype(jnp.bfloat16)
    return high, (value - high.astype(jnp.float32)).astype(jnp.bfloat16)


def dot(left, right):
    return jnp.dot(left, right, preferred_element_type=jnp.float32)


def along_y(real, imag, table_ref):
    straight = jnp.concatenate([real, imag], axis=1)
    half = NY // 2
    data = jnp.concatenate([straight, jnp.concatenate([straight[half:], straight[:half]], axis=0)], axis=1)
    high, low = pieces(data)
    r = dot(table_ref[0], high) + (dot(table_ref[0], low) + dot(table_ref[1], high))
    by_real = r[:half]
    by_imag = r[half:]
    reals = [by_real[:, j : j + 128] - by_imag[:, j + 128 : j + 256] for j in (0, 256)]
    imags = [by_real[:, j + 128 : j + 256] + by_imag[:, j : j + 128] for j in (0, 256)]
    return reals, imags


def along_t(blocks, table_ref):
    rows = blocks[0][0].shape[0]
    split_blocks = [[pieces(block) for block in part] for part in blocks]

    def pairs(k):
        return jnp.concatenate(
            [
                jnp.concatenate([split_blocks[p][g][k], split_blocks[p][(g + 1) % 4][k]], axis=1)
                for g in range(4)
                for p in range(2)
            ],
            axis=0,
        )

    high, low = pairs(0), pairs(1)
    r = dot(high, table_ref[0]) + (dot(low, table_ref[0]) + dot(high, table_ref[1]))

    def product(g, p):
        upper = (2 * g + p) * rows
        lower = (2 * ((g + 2) % 4) + p) * rows
        return r[upper : upper + rows, :256] + r[lower : lower + rows, 256:]

    outs = [[], []]
    for g in range(4):
        from_real = product(g, 0)
        from_imag = product(g, 1)
        outs[0].append(from_real[:, :128] - from_imag[:, 128:])
        outs[1].append(from_imag[:, :128] + from_real[:, 128:])
    return outs


def turns(half):
    count = jnp.floor(half * (1.0 / math.pi) + 0.5)
    rest = ((half - count * 3.140625) - count * 9.67502593994140625e-4) - count * 1.509957990978376432e-7
    square = rest * rest
    sine = rest + (rest * square) * (
        -1.66666563e-1 + square * (8.33299813e-3 + square * (-1.98052344e-4 + square * 2.59701156e-6))
    )
    cosine = 1.0 + square * (
        -4.99999268e-1 + square * (4.16638274e-2 + square * (-1.38546172e-3 + square * 2.31630858e-5))
    )
    twice = sine + sine
    return 1.0 - twice * sine, twice * cosine


def first_kernel(field_hbm, table_hbm, out_ref, field_ref, table_ref, sems):
    copies = [
        pltpu.make_async_copy(field_hbm, field_ref, sems.at[0]),
        pltpu.make_async_copy(table_hbm, table_ref, sems.at[1]),
    ]
    for copy in copies:
        copy.start()
    for copy in copies:
        copy.wait()
    real = field_ref[0]
    imag = field_ref[1]
    reals, imags = along_y(real, imag, table_ref)
    half = NY // 2
    for j in range(2):
        out_ref[pl.ds(3 * half * j, half, stride=3), :] = reals[j]
        out_ref[pl.ds(3 * half * j + 1, half, stride=3), :] = imags[j]
    power = jnp.sum(real * real + imag * imag, axis=0, keepdims=True)
    out_ref[pl.ds(2, NY, stride=3), :] = jnp.broadcast_to(power, (NY, 128))


def time_kernel(in_ref, table_ref, out_ref):
    blocks = [[in_ref[rows_of(g, p, 3), :] for g in range(4)] for p in range(2)]
    outs = along_t(blocks, table_ref)
    for p in range(2):
        for g in range(4):
            out_ref[p * HALF_X : (p + 1) * HALF_X, 128 * g : 128 * (g + 1)] = outs[p][g]
    power = jnp.sum(in_ref[pl.ds(2, NY, stride=3), :], axis=0, keepdims=True)
    out_ref[NX:, :128] = jnp.broadcast_to(power, (8, 128))


def kick_kernel(mine_ref, other_ref, x_table_ref, t_table_ref, out_ref):
    core = lax.axis_index("c")
    position = position_of(lax.axis_index(("z", "x", "h")), lax.axis_index("t"))
    place_y = (position.astype(jnp.float32) - (NY - 1) / 2.0) / (NY / 2.0)
    total = jnp.sum(mine_ref[NX : NX + 1, :128] + other_ref[NX : NX + 1, :128], axis=1, keepdims=True)
    scale = 1.0 / jnp.sqrt(total * (1.0 / (NX * NY * NT)) + EPSILON)
    table = x_table_ref[0, core]
    table_low = x_table_ref[1, core]
    own, own_low = [jnp.concatenate([t[:HALF_X], t[NX : NX + HALF_X]], axis=0) for t in (table, table_low)]
    width = NT // 2
    half_kerr = (0.5 * KERR) * scale * scale
    low_run = spread(lax.broadcasted_iota(jnp.int32, (8, 128), 0))
    half_wells = []
    for start in range(0, NX, 8):
        x = 2 * (low_run ^ run_at(start % HALF_X)) + (core if start < HALF_X else 1 - core)
        place_x = (x.astype(jnp.float32) - (NX - 1) / 2.0) / (NX / 2.0)
        half_well = (0.5 * WELL) * (place_x * place_x + place_y * place_y)
        half_wells.append(jnp.concatenate([half_well] * (width // 128), axis=1))

    def along_x(b):
        parts = [
            ref[p * HALF_X : (p + 1) * HALF_X, b * width : (b + 1) * width]
            for p in range(2)
            for ref in (mine_ref, other_ref)
        ]
        high, low = pieces(jnp.concatenate(parts, axis=0))
        return dot(table, high) + (dot(table, low) + dot(table_low, high))

    def kick(first):
        reals = []
        imags = []
        for start in range(0, NX, 8):
            real = first[start : start + 8]
            imag = first[NX + start : NX + start + 8]
            cos_turn, sin_turn = turns(half_kerr * (real * real + imag * imag) - half_wells[start // 8])
            reals.append(real * cos_turn - imag * sin_turn)
            imags.append(real * sin_turn + imag * cos_turn)
        return jnp.concatenate(reals + imags, axis=0)

    def along_x_own(kicked):
        high, low = pieces(kicked)
        return dot(own, high) + (dot(own, low) + dot(own_low, high))

    firsts = [along_x(0), along_x(1)]
    seconds = [along_x_own(kick(first)) for first in firsts]
    blocks = [
        [seconds[g // 2][p * HALF_X : (p + 1) * HALF_X, 128 * (g % 2) : 128 * (g % 2 + 1)] for g in range(4)]
        for p in range(2)
    ]
    outs = along_t(blocks, t_table_ref)
    for p in range(2):
        for g in range(4):
            out_ref[rows_of(g, p, 2), :] = outs[p][g] * scale


def last_kernel(in_ref, table_ref, out_hbm, out_ref, sems):
    half = NY // 2
    parts = [[in_ref[pl.ds(2 * half * j + p, half, stride=2), :] for p in range(2)] for j in range(2)]
    halves = [pieces(jnp.concatenate(part, axis=1)) for part in parts]
    copies = []
    for j in range(2):
        high, low = [jnp.concatenate([halves[j][k], halves[1 - j][k]], axis=0) for k in range(2)]
        r = dot(table_ref[0], high) + (dot(table_ref[0], low) + dot(table_ref[1], high))
        rows = pl.ds(j * half, half)
        out_ref[0, rows] = r[:half, :128] - r[half:, 128:]
        out_ref[1, rows] = r[:half, 128:] + r[half:, :128]
        copies.append(pltpu.make_async_copy(out_ref.at[:, rows], out_hbm.at[:, rows], sems.at[j]))
        copies[j].start()
    for copy in copies:
        copy.wait()


def call(kernel, shape, *args, scratch=(), direct=False, out_space=pltpu.VMEM):
    source = pltpu.HBM if direct else pltpu.VMEM
    return pl.pallas_call(
        kernel,
        in_specs=[pl.BlockSpec(memory_space=source) for _ in args],
        out_specs=pl.BlockSpec(memory_space=out_space),
        out_shape=jax.ShapeDtypeStruct(shape, jnp.float32),
        scratch_shapes=list(scratch),
        compiler_params=pltpu.CompilerParams(vmem_limit_bytes=16 * 2**20),
        name=kernel.__name__,
    )(*args)


def groups():
    found = np.empty((2, NY), np.int64)
    for run in range(HALF_X):
        for t in range(4):
            for core in range(2):
                found[core, position_of(run, t)] = run * 8 + core * 4 + t
    return found.tolist()


def to_chips(rows, count):
    moved = lax.all_to_all(
        rows.reshape(NY, 1, count * 128),
        DEVICES,
        split_axis=0,
        concat_axis=0,
        tiled=True,
        axis_index_groups=groups(),
    )
    return moved.reshape(count * NY, 128)


def on_device(field, y_table, t_table, x_table):
    scratch = [pltpu.VMEM((2, NY, 128), jnp.float32), pltpu.VMEM(y_table.shape, jnp.bfloat16), pltpu.SemaphoreType.DMA((2,))]
    from_hbm = [pltpu.with_memory_space_constraint(a, pltpu.HBM) for a in (field.reshape(2, NY, 128), y_table)]
    rows = call(first_kernel, (3 * NY, 128), *from_hbm, scratch=scratch, direct=True)
    mine = call(time_kernel, (NX + 8, NT), to_chips(rows, 3), t_table)
    other = lax.ppermute(mine, "c", [(0, 1), (1, 0)])
    rows = call(kick_kernel, (2 * NY, 128), mine, other, x_table, t_table)
    scratch = [pltpu.VMEM((2, NY, 128), jnp.float32), pltpu.SemaphoreType.DMA((2,))]
    out = call(last_kernel, (2, NY, 128), to_chips(rows, 2), y_table, scratch=scratch, out_space=pltpu.HBM)
    return out.reshape(2, 1, NY, 128)


def solution(mesh):
    torus = Mesh(mesh.devices.reshape(8, 4, 2, 2, mesh.shape["tm"]), DEVICES)
    along_x = propagator(NX, -DIFFRACT)
    runs = run_at(np.arange(HALF_X))
    x_tables = []
    for core in range(2):
        order = np.concatenate([2 * runs + core, 2 * runs + 1 - core])
        x_tables.append(real_block(along_x[order][:, order]))
    y_rows = propagator(NY, -DIFFRACT)[: NY // 2]
    t_columns = propagator(NT, DISPERSE).T[:, :128]
    t_columns = np.concatenate([t_columns.real, t_columns.imag], axis=1)
    tables = (
        split(np.concatenate([y_rows.real, y_rows.imag], axis=0)),
        split(np.concatenate([t_columns[: NT // 2], t_columns[NT // 2 :]], axis=1)),
        np.stack(x_tables, axis=1),
    )
    placed = P(None, SLAB, None, "t")
    inner = jax.shard_map(
        lambda field: on_device(field, *[jnp.asarray(table) for table in tables]),
        mesh=torus,
        in_specs=(placed,),
        out_specs=placed,
        check_vma=False,
    )
    return inner
```

```python
import math

import jax
import jax.numpy as jnp
import ml_dtypes
import numpy as np
from jax import lax
from jax.experimental import pallas as pl
from jax.experimental.pallas import tpu as pltpu
from jax.sharding import Mesh
from jax.sharding import PartitionSpec as P

NX = 128
NY = 256
NT = 512
HALF_X = NX // 2
SLAB = ("z", "x", "h", "c")
DEVICES = ("z", "x", "h", "c", "t")
RUN_BITS = (5, 4, 3, 2, 1, 0)
FLIP = 45
T_HIGH = True

TWO_PI = 2.0 * math.pi
DIFFRACT = 4.0
DISPERSE = 3.0
KERR = 0.05
WELL = 1.5
EPSILON = 1e-06


def propagator(length, weight):
    positions = np.arange(length)
    signed = np.where(2 * positions < length, positions, positions - length)
    angle = weight * (signed * (TWO_PI / length)) ** 2
    kernel = np.fft.ifft(np.exp(1j * angle))
    return kernel[(positions[:, None] - positions[None, :]) % length]


def split(matrix):
    full = matrix.astype(np.float32)
    high = full.astype(ml_dtypes.bfloat16)
    low = (matrix - high.astype(np.float64)).astype(ml_dtypes.bfloat16)
    return np.stack([high, low])


def spread(place):
    return sum(((place >> i) & 1) << bit for i, bit in enumerate(RUN_BITS))


def run_at(place):
    return spread(place) ^ FLIP


def position_of(run, t):
    place = sum((((run ^ FLIP) >> bit) & 1) << i for i, bit in enumerate(RUN_BITS))
    return t * HALF_X + place if T_HIGH else 4 * place + t


def rows_of(t, part, count):
    if T_HIGH:
        return pl.ds(count * HALF_X * t + part, HALF_X, stride=count)
    return pl.ds(count * t + part, HALF_X, stride=4 * count)


def real_block(matrix):
    return split(np.block([[matrix.real, -matrix.imag], [matrix.imag, matrix.real]]))


def pieces(value):
    high = value.astype(jnp.bfloat16)
    return high, (value - high.astype(jnp.float32)).astype(jnp.bfloat16)


def dot(left, right):
    return jnp.dot(left, right, preferred_element_type=jnp.float32)


def along_y(real, imag, table_ref):
    straight = jnp.concatenate([real, imag], axis=1)
    half = NY // 2
    data = jnp.concatenate([straight, jnp.concatenate([straight[half:], straight[:half]], axis=0)], axis=1)
    high, low = pieces(data)
    r = dot(table_ref[0], high) + (dot(table_ref[0], low) + dot(table_ref[1], high))
    by_real = r[:half]
    by_imag = r[half:]
    reals = [by_real[:, j : j + 128] - by_imag[:, j + 128 : j + 256] for j in (0, 256)]
    imags = [by_real[:, j + 128 : j + 256] + by_imag[:, j : j + 128] for j in (0, 256)]
    return reals, imags


def along_t(blocks, table_ref):
    rows = blocks[0][0].shape[0]
    split_blocks = [[pieces(block) for block in part] for part in blocks]

    def pairs(k):
        return jnp.concatenate(
            [
                jnp.concatenate([split_blocks[p][g][k], split_blocks[p][(g + 1) % 4][k]], axis=1)
                for g in range(4)
                for p in range(2)
            ],
            axis=0,
        )

    high, low = pairs(0), pairs(1)
    r = dot(high, table_ref[0]) + (dot(low, table_ref[0]) + dot(high, table_ref[1]))

    def product(g, p):
        upper = (2 * g + p) * rows
        lower = (2 * ((g + 2) % 4) + p) * rows
        return r[upper : upper + rows, :256] + r[lower : lower + rows, 256:]

    outs = [[], []]
    for g in range(4):
        from_real = product(g, 0)
        from_imag = product(g, 1)
        outs[0].append(from_real[:, :128] - from_imag[:, 128:])
        outs[1].append(from_imag[:, :128] + from_real[:, 128:])
    return outs


def turns(half):
    count = jnp.floor(half * (1.0 / math.pi) + 0.5)
    rest = ((half - count * 3.140625) - count * 9.67502593994140625e-4) - count * 1.509957990978376432e-7
    square = rest * rest
    sine = rest + (rest * square) * (
        -1.66666563e-1 + square * (8.33299813e-3 + square * (-1.98052344e-4 + square * 2.59701156e-6))
    )
    cosine = 1.0 + square * (
        -4.99999268e-1 + square * (4.16638274e-2 + square * (-1.38546172e-3 + square * 2.31630858e-5))
    )
    twice = sine + sine
    return 1.0 - twice * sine, twice * cosine


def first_kernel(field_hbm, table_hbm, out_ref, field_ref, table_ref, sems):
    copies = [
        pltpu.make_async_copy(field_hbm, field_ref, sems.at[0]),
        pltpu.make_async_copy(table_hbm, table_ref, sems.at[1]),
    ]
    for copy in copies:
        copy.start()
    for copy in copies:
        copy.wait()
    real = field_ref[0]
    imag = field_ref[1]
    reals, imags = along_y(real, imag, table_ref)
    half = NY // 2
    for j in range(2):
        out_ref[pl.ds(3 * half * j, half, stride=3), :] = reals[j]
        out_ref[pl.ds(3 * half * j + 1, half, stride=3), :] = imags[j]
    power = jnp.sum(real * real + imag * imag, axis=0, keepdims=True)
    out_ref[pl.ds(2, NY, stride=3), :] = jnp.broadcast_to(power, (NY, 128))


def time_kernel(in_ref, table_ref, out_ref):
    blocks = [[in_ref[rows_of(g, p, 3), :] for g in range(4)] for p in range(2)]
    outs = along_t(blocks, table_ref)
    for p in range(2):
        for g in range(4):
            out_ref[p * HALF_X : (p + 1) * HALF_X, 128 * g : 128 * (g + 1)] = outs[p][g]
    power = jnp.sum(in_ref[pl.ds(2, NY, stride=3), :], axis=0, keepdims=True)
    out_ref[NX:, :128] = jnp.broadcast_to(power, (8, 128))


def kick_kernel(mine_ref, other_ref, x_table_ref, t_table_ref, out_ref):
    core = lax.axis_index("c")
    position = position_of(lax.axis_index(("z", "x", "h")), lax.axis_index("t"))
    place_y = (position.astype(jnp.float32) - (NY - 1) / 2.0) / (NY / 2.0)
    total = jnp.sum(mine_ref[NX : NX + 1, :128] + other_ref[NX : NX + 1, :128], axis=1, keepdims=True)
    scale = 1.0 / jnp.sqrt(total * (1.0 / (NX * NY * NT)) + EPSILON)
    table = x_table_ref[0, core]
    table_low = x_table_ref[1, core]
    own, own_low = [jnp.concatenate([t[:HALF_X], t[NX : NX + HALF_X]], axis=0) for t in (table, table_low)]
    width = NT // 2
    half_kerr = (0.5 * KERR) * scale * scale
    low_run = spread(lax.broadcasted_iota(jnp.int32, (8, 128), 0))
    half_wells = []
    for start in range(0, NX, 8):
        x = 2 * (low_run ^ run_at(start % HALF_X)) + (core if start < HALF_X else 1 - core)
        place_x = (x.astype(jnp.float32) - (NX - 1) / 2.0) / (NX / 2.0)
        half_well = (0.5 * WELL) * (place_x * place_x + place_y * place_y)
        half_wells.append(jnp.concatenate([half_well] * (width // 128), axis=1))

    def along_x(b):
        parts = [
            ref[p * HALF_X : (p + 1) * HALF_X, b * width : (b + 1) * width]
            for p in range(2)
            for ref in (mine_ref, other_ref)
        ]
        high, low = pieces(jnp.concatenate(parts, axis=0))
        return dot(table, high) + (dot(table, low) + dot(table_low, high))

    def kick(first):
        reals = []
        imags = []
        for start in range(0, NX, 8):
            real = first[start : start + 8]
            imag = first[NX + start : NX + start + 8]
            cos_turn, sin_turn = turns(half_kerr * (real * real + imag * imag) - half_wells[start // 8])
            reals.append(real * cos_turn - imag * sin_turn)
            imags.append(real * sin_turn + imag * cos_turn)
        return jnp.concatenate(reals + imags, axis=0)

    def along_x_own(kicked):
        high, low = pieces(kicked)
        return dot(own, high) + (dot(own, low) + dot(own_low, high))

    firsts = [along_x(0), along_x(1)]
    seconds = [along_x_own(kick(first)) for first in firsts]
    blocks = [
        [seconds[g // 2][p * HALF_X : (p + 1) * HALF_X, 128 * (g % 2) : 128 * (g % 2 + 1)] for g in range(4)]
        for p in range(2)
    ]
    outs = along_t(blocks, t_table_ref)
    for p in range(2):
        for g in range(4):
            out_ref[rows_of(g, p, 2), :] = outs[p][g] * scale


def last_kernel(in_ref, table_ref, out_ref):
    real = in_ref[pl.ds(0, NY, stride=2), :]
    imag = in_ref[pl.ds(1, NY, stride=2), :]
    reals, imags = along_y(real, imag, table_ref)
    half = NY // 2
    for j in range(2):
        out_ref[0, j * half : (j + 1) * half] = reals[j]
        out_ref[1, j * half : (j + 1) * half] = imags[j]


def call(kernel, shape, *args, scratch=(), direct=False):
    source = pltpu.HBM if direct else pltpu.VMEM
    return pl.pallas_call(
        kernel,
        in_specs=[pl.BlockSpec(memory_space=source) for _ in args],
        out_specs=pl.BlockSpec(memory_space=pltpu.VMEM),
        out_shape=jax.ShapeDtypeStruct(shape, jnp.float32),
        scratch_shapes=list(scratch),
        compiler_params=pltpu.CompilerParams(vmem_limit_bytes=16 * 2**20),
        name=kernel.__name__,
    )(*args)


def groups():
    found = np.empty((2, NY), np.int64)
    for run in range(HALF_X):
        for t in range(4):
            for core in range(2):
                found[core, position_of(run, t)] = run * 8 + core * 4 + t
    return found.tolist()


def to_chips(rows, count):
    moved = lax.all_to_all(
        rows.reshape(NY, 1, count * 128),
        DEVICES,
        split_axis=0,
        concat_axis=0,
        tiled=True,
        axis_index_groups=groups(),
    )
    return moved.reshape(count * NY, 128)


def on_device(field, y_table, t_table, x_table):
    scratch = [pltpu.VMEM((2, NY, 128), jnp.float32), pltpu.VMEM(y_table.shape, jnp.bfloat16), pltpu.SemaphoreType.DMA((2,))]
    from_hbm = [pltpu.with_memory_space_constraint(a, pltpu.HBM) for a in (field.reshape(2, NY, 128), y_table)]
    rows = call(first_kernel, (3 * NY, 128), *from_hbm, scratch=scratch, direct=True)
    mine = call(time_kernel, (NX + 8, NT), to_chips(rows, 3), t_table)
    other = lax.ppermute(mine, "c", [(0, 1), (1, 0)])
    rows = call(kick_kernel, (2 * NY, 128), mine, other, x_table, t_table)
    out = call(last_kernel, (2, NY, 128), to_chips(rows, 2), y_table)
    return out.reshape(2, 1, NY, 128)


def solution(mesh):
    torus = Mesh(mesh.devices.reshape(8, 4, 2, 2, mesh.shape["tm"]), DEVICES)
    along_x = propagator(NX, -DIFFRACT)
    runs = run_at(np.arange(HALF_X))
    x_tables = []
    for core in range(2):
        order = np.concatenate([2 * runs + core, 2 * runs + 1 - core])
        x_tables.append(real_block(along_x[order][:, order]))
    y_rows = propagator(NY, -DIFFRACT)[: NY // 2]
    t_columns = propagator(NT, DISPERSE).T[:, :128]
    t_columns = np.concatenate([t_columns.real, t_columns.imag], axis=1)
    tables = (
        split(np.concatenate([y_rows.real, y_rows.imag], axis=0)),
        split(np.concatenate([t_columns[: NT // 2], t_columns[NT // 2 :]], axis=1)),
        np.stack(x_tables, axis=1),
    )
    placed = P(None, SLAB, None, "t")
    inner = jax.shard_map(
        lambda field: on_device(field, *[jnp.asarray(table) for table in tables]),
        mesh=torus,
        in_specs=(placed,),
        out_specs=placed,
        check_vma=False,
    )
    return inner
```

```python
import math

import jax
import jax.numpy as jnp
import ml_dtypes
import numpy as np
from jax import lax
from jax.experimental import pallas as pl
from jax.experimental.pallas import tpu as pltpu
from jax.sharding import Mesh
from jax.sharding import PartitionSpec as P

NX = 128
NY = 256
NT = 512
HALF_X = NX // 2
SLAB = ("z", "x", "h", "c")
DEVICES = ("z", "x", "h", "c", "t")
RUN_BITS = (5, 4, 3, 2, 1, 0)
FLIP = 37
T_HIGH = True

TWO_PI = 2.0 * math.pi
DIFFRACT = 4.0
DISPERSE = 3.0
KERR = 0.05
WELL = 1.5
EPSILON = 1e-06


def propagator(length, weight):
    positions = np.arange(length)
    signed = np.where(2 * positions < length, positions, positions - length)
    angle = weight * (signed * (TWO_PI / length)) ** 2
    kernel = np.fft.ifft(np.exp(1j * angle))
    return kernel[(positions[:, None] - positions[None, :]) % length]


def split(matrix):
    full = matrix.astype(np.float32)
    high = full.astype(ml_dtypes.bfloat16)
    low = (matrix - high.astype(np.float64)).astype(ml_dtypes.bfloat16)
    return np.stack([high, low])


def spread(place):
    return sum(((place >> i) & 1) << bit for i, bit in enumerate(RUN_BITS))


def run_at(place):
    return spread(place) ^ FLIP


def position_of(run, t):
    place = sum((((run ^ FLIP) >> bit) & 1) << i for i, bit in enumerate(RUN_BITS))
    return t * HALF_X + place if T_HIGH else 4 * place + t


def rows_of(t, part, count):
    if T_HIGH:
        return pl.ds(count * HALF_X * t + part, HALF_X, stride=count)
    return pl.ds(count * t + part, HALF_X, stride=4 * count)


def real_block(matrix):
    return split(np.block([[matrix.real, -matrix.imag], [matrix.imag, matrix.real]]))


def pieces(value):
    high = value.astype(jnp.bfloat16)
    return high, (value - high.astype(jnp.float32)).astype(jnp.bfloat16)


def dot(left, right):
    return jnp.dot(left, right, preferred_element_type=jnp.float32)


def along_y(real, imag, table_ref):
    straight = jnp.concatenate([real, imag], axis=1)
    half = NY // 2
    data = jnp.concatenate([straight, jnp.concatenate([straight[half:], straight[:half]], axis=0)], axis=1)
    high, low = pieces(data)
    r = dot(table_ref[0], high) + (dot(table_ref[0], low) + dot(table_ref[1], high))
    by_real = r[:half]
    by_imag = r[half:]
    reals = [by_real[:, j : j + 128] - by_imag[:, j + 128 : j + 256] for j in (0, 256)]
    imags = [by_real[:, j + 128 : j + 256] + by_imag[:, j : j + 128] for j in (0, 256)]
    return reals, imags


def along_t(blocks, table_ref):
    rows = blocks[0][0].shape[0]
    split_blocks = [[pieces(block) for block in part] for part in blocks]

    def pairs(k):
        return jnp.concatenate(
            [
                jnp.concatenate([split_blocks[p][g][k], split_blocks[p][(g + 1) % 4][k]], axis=1)
                for g in range(4)
                for p in range(2)
            ],
            axis=0,
        )

    high, low = pairs(0), pairs(1)
    r = dot(high, table_ref[0]) + (dot(low, table_ref[0]) + dot(high, table_ref[1]))

    def product(g, p):
        upper = (2 * g + p) * rows
        lower = (2 * ((g + 2) % 4) + p) * rows
        return r[upper : upper + rows, :256] + r[lower : lower + rows, 256:]

    outs = [[], []]
    for g in range(4):
        from_real = product(g, 0)
        from_imag = product(g, 1)
        outs[0].append(from_real[:, :128] - from_imag[:, 128:])
        outs[1].append(from_imag[:, :128] + from_real[:, 128:])
    return outs


def turns(half):
    count = jnp.round(half * (1.0 / math.pi))
    rest = ((half - count * 3.140625) - count * 9.67502593994140625e-4) - count * 1.509957990978376432e-7
    square = rest * rest
    sine = rest + (rest * square) * (
        -1.66666563e-1 + square * (8.33299813e-3 + square * (-1.98052344e-4 + square * 2.59701156e-6))
    )
    cosine = 1.0 + square * (
        -4.99999268e-1 + square * (4.16638274e-2 + square * (-1.38546172e-3 + square * 2.31630858e-5))
    )
    twice = sine + sine
    return 1.0 - twice * sine, twice * cosine


def first_kernel(field_hbm, table_hbm, out_ref, field_ref, table_ref, sems):
    copies = [
        pltpu.make_async_copy(field_hbm, field_ref, sems.at[0]),
        pltpu.make_async_copy(table_hbm, table_ref, sems.at[1]),
    ]
    for copy in copies:
        copy.start()
    for copy in copies:
        copy.wait()
    real = field_ref[0]
    imag = field_ref[1]
    reals, imags = along_y(real, imag, table_ref)
    half = NY // 2
    for j in range(2):
        out_ref[pl.ds(3 * half * j, half, stride=3), :] = reals[j]
        out_ref[pl.ds(3 * half * j + 1, half, stride=3), :] = imags[j]
    power = jnp.sum(real * real + imag * imag, axis=0, keepdims=True)
    out_ref[pl.ds(2, NY, stride=3), :] = jnp.broadcast_to(power, (NY, 128))


def time_kernel(in_ref, table_ref, out_ref):
    blocks = [[in_ref[rows_of(g, p, 3), :] for g in range(4)] for p in range(2)]
    outs = along_t(blocks, table_ref)
    for p in range(2):
        for g in range(4):
            out_ref[p * HALF_X : (p + 1) * HALF_X, 128 * g : 128 * (g + 1)] = outs[p][g]
    power = jnp.sum(in_ref[pl.ds(2, NY, stride=3), :], axis=0, keepdims=True)
    out_ref[NX:, :128] = jnp.broadcast_to(power, (8, 128))


def kick_kernel(mine_ref, other_ref, x_table_ref, t_table_ref, out_ref):
    core = lax.axis_index("c")
    position = position_of(lax.axis_index(("z", "x", "h")), lax.axis_index("t"))
    place_y = (position.astype(jnp.float32) - (NY - 1) / 2.0) / (NY / 2.0)
    total = jnp.sum(mine_ref[NX : NX + 1, :128] + other_ref[NX : NX + 1, :128], axis=1, keepdims=True)
    scale = 1.0 / jnp.sqrt(total * (1.0 / (NX * NY * NT)) + EPSILON)
    table = x_table_ref[0, core]
    table_low = x_table_ref[1, core]
    own, own_low = [jnp.concatenate([t[:HALF_X], t[NX : NX + HALF_X]], axis=0) for t in (table, table_low)]
    width = NT // 2
    half_kerr = (0.5 * KERR) * scale * scale
    low_run = spread(lax.broadcasted_iota(jnp.int32, (8, 128), 0))
    half_wells = []
    for start in range(0, NX, 8):
        x = 2 * (low_run ^ run_at(start % HALF_X)) + (core if start < HALF_X else 1 - core)
        place_x = (x.astype(jnp.float32) - (NX - 1) / 2.0) / (NX / 2.0)
        half_well = (0.5 * WELL) * (place_x * place_x + place_y * place_y)
        half_wells.append(jnp.concatenate([half_well] * (width // 128), axis=1))

    def along_x(b):
        parts = [
            ref[p * HALF_X : (p + 1) * HALF_X, b * width : (b + 1) * width]
            for p in range(2)
            for ref in (mine_ref, other_ref)
        ]
        high, low = pieces(jnp.concatenate(parts, axis=0))
        return dot(table, high) + (dot(table, low) + dot(table_low, high))

    def kick(first):
        reals = []
        imags = []
        for start in range(0, NX, 8):
            real = first[start : start + 8]
            imag = first[NX + start : NX + start + 8]
            cos_turn, sin_turn = turns(half_kerr * (real * real + imag * imag) - half_wells[start // 8])
            reals.append(real * cos_turn - imag * sin_turn)
            imags.append(real * sin_turn + imag * cos_turn)
        return jnp.concatenate(reals + imags, axis=0)

    def along_x_own(kicked):
        high, low = pieces(kicked)
        return dot(own, high) + (dot(own, low) + dot(own_low, high))

    firsts = [along_x(0), along_x(1)]
    seconds = [along_x_own(kick(first)) for first in firsts]
    blocks = [
        [seconds[g // 2][p * HALF_X : (p + 1) * HALF_X, 128 * (g % 2) : 128 * (g % 2 + 1)] for g in range(4)]
        for p in range(2)
    ]
    outs = along_t(blocks, t_table_ref)
    for p in range(2):
        for g in range(4):
            out_ref[rows_of(g, p, 2), :] = outs[p][g] * scale


def last_kernel(in_ref, table_ref, out_ref):
    real = in_ref[pl.ds(0, NY, stride=2), :]
    imag = in_ref[pl.ds(1, NY, stride=2), :]
    reals, imags = along_y(real, imag, table_ref)
    half = NY // 2
    for j in range(2):
        out_ref[0, j * half : (j + 1) * half] = reals[j]
        out_ref[1, j * half : (j + 1) * half] = imags[j]


def call(kernel, shape, *args, scratch=(), direct=False):
    source = pltpu.HBM if direct else pltpu.VMEM
    return pl.pallas_call(
        kernel,
        in_specs=[pl.BlockSpec(memory_space=source) for _ in args],
        out_specs=pl.BlockSpec(memory_space=pltpu.VMEM),
        out_shape=jax.ShapeDtypeStruct(shape, jnp.float32),
        scratch_shapes=list(scratch),
        compiler_params=pltpu.CompilerParams(vmem_limit_bytes=16 * 2**20),
        name=kernel.__name__,
    )(*args)


def groups():
    found = np.empty((2, NY), np.int64)
    for run in range(HALF_X):
        for t in range(4):
            for core in range(2):
                found[core, position_of(run, t)] = run * 8 + core * 4 + t
    return found.tolist()


def to_chips(rows, count):
    moved = lax.all_to_all(
        rows.reshape(NY, 1, count * 128),
        DEVICES,
        split_axis=0,
        concat_axis=0,
        tiled=True,
        axis_index_groups=groups(),
    )
    return moved.reshape(count * NY, 128)


def on_device(field, y_table, t_table, x_table):
    scratch = [pltpu.VMEM((2, NY, 128), jnp.float32), pltpu.VMEM(y_table.shape, jnp.bfloat16), pltpu.SemaphoreType.DMA((2,))]
    from_hbm = [pltpu.with_memory_space_constraint(a, pltpu.HBM) for a in (field.reshape(2, NY, 128), y_table)]
    rows = call(first_kernel, (3 * NY, 128), *from_hbm, scratch=scratch, direct=True)
    mine = call(time_kernel, (NX + 8, NT), to_chips(rows, 3), t_table)
    other = lax.ppermute(mine, "c", [(0, 1), (1, 0)])
    rows = call(kick_kernel, (2 * NY, 128), mine, other, x_table, t_table)
    out = call(last_kernel, (2, NY, 128), to_chips(rows, 2), y_table)
    return out.reshape(2, 1, NY, 128)


def solution(mesh):
    torus = Mesh(mesh.devices.reshape(8, 4, 2, 2, mesh.shape["tm"]), DEVICES)
    along_x = propagator(NX, -DIFFRACT)
    runs = run_at(np.arange(HALF_X))
    x_tables = []
    for core in range(2):
        order = np.concatenate([2 * runs + core, 2 * runs + 1 - core])
        x_tables.append(real_block(along_x[order][:, order]))
    y_rows = propagator(NY, -DIFFRACT)[: NY // 2]
    t_columns = propagator(NT, DISPERSE).T[:, :128]
    t_columns = np.concatenate([t_columns.real, t_columns.imag], axis=1)
    tables = (
        split(np.concatenate([y_rows.real, y_rows.imag], axis=0)),
        split(np.concatenate([t_columns[: NT // 2], t_columns[NT // 2 :]], axis=1)),
        np.stack(x_tables, axis=1),
    )
    placed = P(None, SLAB, None, "t")
    inner = jax.shard_map(
        lambda field: on_device(field, *[jnp.asarray(table) for table in tables]),
        mesh=torus,
        in_specs=(placed,),
        out_specs=placed,
        check_vma=False,
    )
    return inner
```
